256 devices in a mesh: ga: 32 (over z, x), band: 8 (over y, core).
Axes of the slice: x: 4, y: 4, z: 8, core: 2. Of those that a mesh axis runs over, the one named last changes fastest.
Arguments:
- waves: float32 [2, 32768, 2048], P(None, 'ga', 'band'), may hold values from -6 to 6
- miller: int32 [3, 32768], P(None, 'ga'), may hold values from -8 to 8
- positions: float32 [64, 3], replicated, may hold values from 0 to 1
- form_factors: float32 [4, 18, 32768], P(None, None, 'ga'), may hold values from -0.03125 to 0.03125
- coupling: float32 [4, 18, 18], replicated, may hold values from -3.3941125 to 11.313708
- species: int32 [64], replicated, may hold values from 0 to 3
- block_sizes: int32 [64], replicated, may hold values from 1 to 18, 512 in all
- occupation: float32 [2048], P('band'), may hold values from 0.05 to 2
Outputs:
- residual: float32 [2, 32768, 2048], P(None, 'ga', 'band')
- estimate: float32 [2048], P('band')
- energy: float32 [], replicated
The draws below stay inside these ranges and needn't reach their ends.
All inputs are finite; a program needn't handle non-finite values.
Results may differ from the reference program's by a relative error of at most 0.00007.
Values sent between devices are 32-bit elements; how exact they have to be, the bound alone decides.
A program may use at most 64 MiB of HBM per device.

```python
import math
import jax
import jax.numpy as jnp
import numpy as np
from jax import lax

ATOMS = 64
KMAX = 18
NSPEC = 4
PROJ = 512
NG = 32768
NB = 2048


def draw_coupling(key, part):
    scale = (NG / (8.0 * PROJ)) ** 0.5
    first_key, second_key = jax.random.split(jax.random.fold_in(key, 11))
    offdiag = jnp.clip(0.3 * jax.random.normal(first_key, (NSPEC, KMAX, KMAX), jnp.float32), -1.2, 1.2)
    diagonal = jnp.exp(jax.random.uniform(second_key, (NSPEC, KMAX), jnp.float32, 0.0, math.log(4.0)))
    identity = jnp.eye(KMAX, dtype=jnp.float32)
    return scale * (offdiag * (1.0 - identity) + diagonal[:, :, None] * identity)


def plant(result, rng, least, top_value):
    dims = result.shape
    index_at = [jax.random.randint(jax.random.fold_in(rng, axis), (), 0, dims[axis]) for axis in range(len(dims))]
    result = result.at[tuple(index_at)].set(least)
    longest = dims.index(max(dims))
    index_at[longest] = (index_at[longest] + 1) % dims[longest]
    return result.at[tuple(index_at)].set(top_value)


def raised(result, own_key, source, target, parts, factor):
    owner, partner = [(jnp.arange(result.shape[position]) // (result.shape[position] // parts)).reshape([-1 if axis == position else 1 for axis in range(result.ndim)]) for position in (source, target)]
    chosen = jax.random.permutation(own_key, parts)[partner]
    strong = (owner == chosen) | (owner == (partner + parts // 2) % parts)
    return jnp.where(strong, factor * result, result)


def shard_levels(key, extent, cuts, low, top_value):
    def one(dim, shards_of):
        draws = jax.random.uniform(jax.random.fold_in(jax.random.fold_in(key, 6), dim), (shards_of,), jnp.float32, low / len(cuts), top_value / len(cuts))
        return jnp.repeat(jnp.exp(draws), extent[dim] // shards_of).reshape((-1,) + (1,) * (len(extent) - dim - 1))

    level = one(*cuts[0])
    for cut in cuts[1:]:
        level = level * one(*cut)
    return level


def profile(amount, total, bound, lean):
    portions = [(1 << 20) // math.isqrt(grade ** lean) + 1 for grade in range(2, amount + 1)]
    rest, holding = total - bound - (amount - 1), [1] * (amount - 1)
    while rest > 0:
        movable = [i for i in range(amount - 1) if holding[i] < bound]
        mass, left = sum([portions[i] for i in movable]), rest
        for i in movable:
            extra = min(bound - holding[i], max(1, left * portions[i] // mass), rest)
            holding[i] = holding[i] + extra
            rest = rest - extra
    return np.array([bound] + holding)


def uneven_parts(stream_key, amount, total, bound, skew):
    if amount == 2:
        one = jax.random.randint(stream_key, (), max(1, total - bound), min(bound, total - 1) + 1)
        return jnp.stack([one, total - one])
    tallies = jnp.asarray(profile(amount, total, bound, skew), jnp.int32)
    pairs = (amount - 1) // 2
    giver, receiver = tallies[1:1 + 2 * pairs:2], tallies[2:2 + 2 * pairs:2]
    slack = jnp.minimum(giver - 1, bound - receiver)
    moved = jax.random.randint(jax.random.fold_in(stream_key, 1), (pairs,), 0, 1 << 20) % (slack + 1)
    tallies = tallies.at[1:1 + 2 * pairs:2].set(giver - moved).at[2:2 + 2 * pairs:2].set(receiver + moved)
    return tallies[jax.random.permutation(jax.random.fold_in(stream_key, 2), amount)]


def scatter_about(rng, shape, spread, reach, cuts=(), kind=jnp.bfloat16):
    entries = spread * jax.random.normal(rng, shape, jnp.float32)
    if cuts:
        entries = entries * shard_levels(rng, shape, cuts, -0.22, 0.18)
    return jnp.clip(entries, -reach, reach).astype(kind)


def heavy_noise(own_key, dims, deviation, reach, cuts, heavy, kind=jnp.bfloat16):
    array = deviation * jax.random.normal(own_key, dims, jnp.float32)
    if cuts:
        array = array * shard_levels(own_key, dims, cuts, -0.22, 0.18)
    return jnp.clip(raised(array, jax.random.fold_in(own_key, 3), *heavy), -reach, reach).astype(kind)


def setup_inputs(seed: int = 0) -> dict:
    streams_of = jax.random.split(jax.random.key(seed), 9)
    waves = heavy_noise(streams_of[0], (2, NG, NB), 1.0, 6.0, ((1, 32), (2, 8)), (1, 2, 32, 2.75), jnp.float32)
    miller = plant(jax.random.randint(streams_of[1], (3, NG), -8, 9), jax.random.fold_in(streams_of[1], 1), -8, 8).astype(jnp.int32)
    positions = jnp.clip(jax.random.uniform(streams_of[2], (ATOMS, 3), jnp.float32, 0.0, 1.0), 0.0, 1.0)
    form_factors = scatter_about(streams_of[3], (NSPEC, KMAX, NG), NG ** -0.5, 0.03125, ((2, 32),), jnp.float32)
    coupling = draw_coupling(jax.random.fold_in(streams_of[8], 71), 0)
    species = plant(jax.random.randint(streams_of[5], (ATOMS,), 0, NSPEC), jax.random.fold_in(streams_of[5], 1), 0, NSPEC - 1).astype(jnp.int32)
    block_sizes = uneven_parts(streams_of[6], ATOMS, PROJ, KMAX, 1).astype(jnp.int32)
    occupation = jnp.clip(jnp.exp(math.log(2.0) - 3.6888794 * jax.random.uniform(streams_of[7], (NB,), jnp.float32) ** shard_levels(streams_of[7], (NB,), ((0, 8),), -0.2, 0.2)), 0.05, 2.0)
    return dict(waves=waves, miller=miller, positions=positions, form_factors=form_factors, coupling=coupling, species=species, block_sizes=block_sizes, occupation=occupation)


TWO_PI = 6.283185307179586
KINETIC_SCALE = 0.005
EPSILON = 1e-6
HIGHEST_PRECISION = lax.Precision.HIGHEST


def reference(waves, miller, positions, form_factors, coupling, species, block_sizes, occupation):
    block_ends = jnp.cumsum(block_sizes).astype(jnp.int32)
    block_starts = (block_ends - block_sizes).astype(jnp.int32)
    columns = jnp.arange(PROJ, dtype=jnp.int32)
    owner_atom = jnp.sum((block_ends[None, :] <= columns[:, None]).astype(jnp.int32), axis=1).astype(jnp.int32)
    channel = (columns - jnp.take(block_starts, owner_atom)).astype(jnp.int32)
    row_index = (jnp.take(species, owner_atom) * KMAX + channel).astype(jnp.int32)
    radial = jnp.take(form_factors.reshape(NSPEC * KMAX, NG), row_index, axis=0)
    miller_f = miller.astype(jnp.float32)
    phases = TWO_PI * (positions[:, 0:1] * miller_f[0][None, :] + positions[:, 1:2] * miller_f[1][None, :] + positions[:, 2:3] * miller_f[2][None, :])
    beta_re = radial * jnp.take(jnp.cos(phases), owner_atom, axis=0)
    beta_im = -(radial * jnp.take(jnp.sin(phases), owner_atom, axis=0))
    table = jnp.take(coupling.reshape(NSPEC * KMAX, KMAX), row_index, axis=0)
    dense = jnp.take(table, channel, axis=1)
    dense = jnp.where(owner_atom[:, None] == owner_atom[None, :], dense, jnp.zeros_like(dense))
    psi_re = waves[0]
    psi_im = waves[1]
    proj_re = jnp.dot(beta_re, psi_re, precision=HIGHEST_PRECISION) + jnp.dot(beta_im, psi_im, precision=HIGHEST_PRECISION)
    proj_im = jnp.dot(beta_re, psi_im, precision=HIGHEST_PRECISION) - jnp.dot(beta_im, psi_re, precision=HIGHEST_PRECISION)
    kinetic = 0.5 * KINETIC_SCALE * (miller_f[0] * miller_f[0] + miller_f[1] * miller_f[1] + miller_f[2] * miller_f[2])
    density = psi_re * psi_re + psi_im * psi_im
    kin_sum = jnp.sum(kinetic[:, None] * density, axis=0)
    norm_sum = jnp.sum(density, axis=0)
    mixed_re = jnp.dot(dense, proj_re, precision=HIGHEST_PRECISION)
    mixed_im = jnp.dot(dense, proj_im, precision=HIGHEST_PRECISION)
    nonlocal_sum = jnp.sum(proj_re * mixed_re + proj_im * mixed_im, axis=0)
    estimate = (kin_sum + nonlocal_sum) / (norm_sum + EPSILON)
    contract = (((0,), (0,)), ((), ()))
    applied_re = lax.dot_general(beta_re, mixed_re, contract, precision=HIGHEST_PRECISION) - lax.dot_general(beta_im, mixed_im, contract, precision=HIGHEST_PRECISION)
    applied_im = lax.dot_general(beta_re, mixed_im, contract, precision=HIGHEST_PRECISION) + lax.dot_general(beta_im, mixed_re, contract, precision=HIGHEST_PRECISION)
    shifted = kinetic[:, None] - estimate[None, :]
    residual = jnp.stack([shifted * psi_re + applied_re, shifted * psi_im + applied_im])
    energy = jnp.sum(occupation * nonlocal_sum / (norm_sum + EPSILON))
    return residual, estimate, energy
```

```python
import jax
import jax.numpy as jnp
from jax import lax
from jax.experimental import pallas as pl
from jax.experimental.pallas import tpu as pltpu
from jax.sharding import PartitionSpec as P

MESH = pl.DeviceIdType.MESH
F32 = jnp.float32
BF16 = jnp.bfloat16

NX = 4
NZ = 8
NBAND = 8
PROJ = 512
ATOMS = 64
NSPEC = 4
KMAX = 18
KPAD = 24
GL = 1024
BL = 256
CH = 128
NCH = BL // CH
QR = PROJ // NX
SR = QR // NZ

KINETIC_SCALE = 0.005
EPSILON = 1e-6

SIN_C = (3.141592653589793, -5.16771278004997, 2.550164039877345, -0.5992645293207921, 0.08214588661112823, -0.00737043094571435, 0.00046630280576761255)
COS_C = (1.0, -4.934802200544679, 4.058712126416768, -1.3352627688545893, 0.2353306303588935, -0.02580689139001406, 0.0019295743094039231)


def split(x):
    hi = x.astype(BF16)
    return hi, (x - hi.astype(F32)).astype(BF16)


def dot(a, b):
    return jnp.dot(a, b, preferred_element_type=F32)


def dot3(ah, al, bh, bl):
    return dot(ah, bh) + dot(al, bh) + dot(ah, bl)


def horner(coeffs, x):
    acc = jnp.full_like(x, coeffs[-1])
    for c in coeffs[-2::-1]:
        acc = acc * x + c
    return acc


def iota(shape, dim):
    return lax.broadcasted_iota(jnp.int32, shape, dim)


def kernel(waves, miller, pos, ff, coup, spec, size, occ,
           res, est_out, en_out,
           psi, bh, bl, th, tl, vh, vl, dh, dl, mh, ml,
           ffk, ctk, stk, ckk, kcol, pbuf, xr, s2, q, zr, full, rbuf,
           knx, knz, kna, ebuf,
           in_sem, out_sem, send, recv):
    gi = lax.axis_index("ga")
    band = lax.axis_index("band")
    z = lax.div(gi, NX)
    x = lax.rem(gi, NX)
    r, o, l = (lax.rem(x + k, NX) for k in (1, 2, 3))

    def at_x(xx):
        return {"ga": z * NX + xx}

    def at_z(k):
        return {"ga": lax.rem(z + k, NZ) * NX + x}

    def at_band(k):
        return {"band": lax.rem(band + k, NBAND)}

    loads = [pltpu.make_async_copy(waves.at[i], psi.at[i], in_sem.at[i]) for i in range(2)]
    for c in loads:
        c.start()

    barrier = pltpu.get_barrier_semaphore()
    peers = [at_x(r), at_x(l), at_x(o)] + [at_z(k) for k in range(1, NZ)] + [at_band(k) for k in range(1, NBAND)]
    for p in peers:
        pl.semaphore_signal(barrier, inc=1, device_id=p, device_id_type=MESH)

    started = []
    slot = [0]

    def remote(src, dst, where):
        i = slot[0]
        slot[0] += 1
        copy = pltpu.make_async_remote_copy(
            src_ref=src, dst_ref=dst, send_sem=send.at[i], recv_sem=recv.at[i],
            device_id=where, device_id_type=MESH,
        )
        started.append(copy)
        copy.start()
        return copy

    def quarter(xx):
        return pl.ds(pl.multiple_of(xx * QR, QR), QR)

    def piece(zz):
        return pl.ds(pl.multiple_of(zz * SR, SR), SR)

    size_row = size[...].astype(F32)
    spec_row = spec[...].astype(F32)
    i0, i1 = iota((ATOMS, ATOMS), 0), iota((ATOMS, ATOMS), 1)
    size_col = jnp.sum(jnp.where(i0 == i1, size_row, 0.0), axis=1, keepdims=True)
    end_row = jnp.sum(jnp.where(i0 <= i1, size_col, 0.0), axis=0, keepdims=True)
    end_col = jnp.sum(jnp.where(i1 <= i0, size_row, 0.0), axis=1, keepdims=True)
    start_row = end_row - size_row
    start_col = end_col - size_col
    p_col = iota((PROJ, ATOMS), 0).astype(F32)
    own = (p_col >= start_row) & (p_col < end_row)
    atom_row = iota((1, ATOMS), 1).astype(F32)
    owner_col = jnp.sum(jnp.where(own, atom_row, 0.0), axis=1, keepdims=True)
    row_col = jnp.sum(jnp.where(own, spec_row * KPAD - start_row + p_col, 0.0), axis=1, keepdims=True)
    lane = iota((PROJ, 256), 1)
    row_hot = jnp.where(lax.rem(lane, 128).astype(F32) == row_col, 1.0, 0.0).astype(BF16)
    own_hot = jnp.where(lax.rem(lane[:, :128], 64).astype(F32) == owner_col, 1.0, 0.0).astype(BF16)

    ffk[...] = jnp.zeros_like(ffk)
    for s in range(NSPEC):
        fh, fl = split(ff[s])
        ffk[s * KPAD:s * KPAD + KMAX, :] = fh
        ffk[128 + s * KPAD:128 + s * KPAD + KMAX, :] = fl
    m = miller[...].astype(F32)
    for g in range(0, GL, 256):
        mg = m[:, g:g + 256]
        turns = pos[:, 0:1] * mg[0:1] + pos[:, 1:2] * mg[1:2] + pos[:, 2:3] * mg[2:3]
        turns = turns - jnp.round(turns)
        t2 = turns * turns
        sh = horner(SIN_C, t2) * turns
        ch = horner(COS_C, t2)
        for dst, val in ((ctk, 1.0 - 2.0 * (sh * sh)), (stk, 2.0 * (sh * ch))):
            a, b = split(val)
            dst[0:64, g:g + 256] = a
            dst[64:128, g:g + 256] = b
        radial = dot(row_hot, ffk[:, g:g + 256])
        for base, tab, sign in ((0, ctk, 1.0), (GL, stk, -1.0)):
            b = radial * dot(own_hot, tab[:, g:g + 256])
            b = b if sign > 0 else -b
            a, b = split(b)
            bh[:, base + g:base + g + 256] = a
            bl[:, base + g:base + g + 256] = b
    ksum = m[0:1] * m[0:1] + m[1:2] * m[1:2] + m[2:3] * m[2:3]
    krow = jnp.broadcast_to(0.5 * KINETIC_SCALE * ksum, (128, GL))
    for g in range(0, GL, 128):
        kcol[g:g + 128, :] = jnp.transpose(krow[:, g:g + 128])

    for c in loads:
        c.wait()

    def project(c):
        cols = slice(c * CH, (c + 1) * CH)
        rows = 256
        kin = jnp.zeros((1, CH), F32)
        nrm = jnp.zeros((1, CH), F32)
        for g in range(0, GL, rows):
            pr = psi[0, g:g + rows, cols]
            pi = psi[1, g:g + rows, cols]
            den = pr * pr + pi * pi
            nrm = nrm + jnp.sum(den, axis=0, keepdims=True)
            kin = kin + jnp.sum(kcol[g:g + rows, :] * den, axis=0, keepdims=True)
            for buf, (a, b) in zip((vh, vl), zip(split(pr), split(pi))):
                buf[g:g + rows, 0:CH] = a
                buf[g:g + rows, CH:2 * CH] = b
                buf[GL + g:GL + g + rows, 0:CH] = b
                buf[GL + g:GL + g + rows, CH:2 * CH] = -a
        p = dot3(bh[...], bl[...], vh[...], vl[...])
        pbuf[c, 0] = p[:, :CH]
        pbuf[c, 1] = p[:, CH:]
        return kin, nrm

    def x_first(c):
        return [
            remote(pbuf.at[c, 0, quarter(o)], xr.at[c, 0], at_x(r)),
            remote(pbuf.at[c, 1, quarter(o)], xr.at[c, 1], at_x(l)),
            remote(pbuf.at[c, 1, quarter(r)], xr.at[c, 2], at_x(r)),
            remote(pbuf.at[c, 0, quarter(l)], xr.at[c, 3], at_x(l)),
        ]

    def x_second(c, first):
        first[0].wait_recv()
        s2[c, 0] = xr[c, 0] + pbuf[c, 0, quarter(r), :]
        a = remote(s2.at[c, 0], xr.at[c, 4], at_x(r))
        first[1].wait_recv()
        s2[c, 1] = xr[c, 1] + pbuf[c, 1, quarter(l), :]
        b = remote(s2.at[c, 1], xr.at[c, 5], at_x(l))
        return [a, b]

    def z_first(c, first, second):
        for w in first[2:] + second:
            w.wait_recv()
        q[c, 0] = pbuf[c, 0, quarter(x), :] + xr[c, 4] + xr[c, 3]
        q[c, 1] = pbuf[c, 1, quarter(x), :] + xr[c, 5] + xr[c, 2]
        return [
            remote(q.at[c, :, piece(lax.rem(z + k, NZ)), :], zr.at[c, k - 1], at_z(k))
            for k in (4, 3, 5, 2, 6, 1, 7)
        ]

    mine = pl.ds(pl.multiple_of(x * QR + z * SR, SR), SR)

    def z_back(c, zs):
        for w in zs:
            w.wait_recv()
        share = q[c, :, piece(z), :]
        for k in range(NZ - 1):
            share = share + zr[c, k]
        full[c, :, mine, :] = share
        return [remote(full.at[c, :, mine, :], full.at[c, :, mine, :], at_z(k)) for k in (4, 3, 5, 2, 6, 1, 7)]

    def x_back(c, zs):
        for w in zs:
            w.wait_recv()
        out = []
        for h, first, then in ((0, r, l), (1, l, r)):
            part = full.at[c, h, quarter(x)]
            out.append(remote(part, part, at_x(first)))
        for h, first, then in ((0, r, l), (1, l, r)):
            part = full.at[c, h, quarter(x)]
            out.append(remote(part, part, at_x(then)))
        return out

    def x_relay(c, xs):
        out = []
        for h, source, to in ((0, l, r), (1, r, l)):
            xs[h].wait_recv()
            part = full.at[c, h, quarter(source)]
            out.append(remote(part, part, at_x(to)))
        return out

    kn0 = project(0)
    pl.semaphore_wait(barrier, len(peers))
    first0 = x_first(0)
    kn1 = project(1)
    first1 = x_first(1)

    tile_row = iota((8, CH), 0)
    kn = jnp.zeros((8, CH), F32)
    for i, v in enumerate((kn0[0], kn0[1], kn1[0], kn1[1])):
        kn = jnp.where(tile_row == i, v, kn)
    knx[x] = kn
    knx_sent = [remote(knx.at[x], knx.at[x], at_x(k)) for k in (r, l, o)]

    second0 = x_second(0, first0)

    for w in knx_sent:
        w.wait_recv()
    knz[z] = knx[0] + knx[1] + knx[2] + knx[3]
    knz_sent = [remote(knz.at[z], knz.at[z], at_z(k)) for k in range(1, NZ)]

    second1 = x_second(1, first1)

    ckk[...] = jnp.zeros_like(ckk)
    for s in range(NSPEC):
        a, b = split(coup[s])
        ckk[s * KPAD:s * KPAD + KMAX, 0:KMAX] = a
        ckk[128 + s * KPAD:128 + s * KPAD + KMAX, 0:KMAX] = b
    q_row = iota((ATOMS, PROJ), 1).astype(F32)
    own_t = (q_row >= start_col) & (q_row < end_col)
    atom_col = iota((ATOMS, 1), 0).astype(F32)
    owner_row = jnp.sum(jnp.where(own_t, atom_col, 0.0), axis=0, keepdims=True)
    chan_row = jnp.sum(jnp.where(own_t, q_row - start_col, 0.0), axis=0, keepdims=True)
    chan_hot = jnp.where(iota((128, PROJ), 0).astype(F32) == chan_row, 1.0, 0.0).astype(BF16)
    same = owner_col == owner_row
    for dst, part in ((dh, row_hot[:, :128]), (dl, row_hot[:, 128:])):
        base = 0 if dst is dh else 128
        table = dot(part, ckk[base:base + 128, :]).astype(BF16)
        dst[...] = jnp.where(same, dot(table, chan_hot), 0.0).astype(BF16)

    zs0 = z_first(0, first0, second0)
    zs1 = z_first(1, first1, second1)

    def turned(g):
        for src, dst in ((bh, th), (bl, tl)):
            for half in range(2):
                dst[g:g + 256, half * PROJ:(half + 1) * PROJ] = jnp.transpose(
                    src[:, half * GL + g:half * GL + g + 256]
                )

    turned(0)
    turned(256)
    zb0 = z_back(0, zs0)
    zb1 = z_back(1, zs1)
    turned(512)
    turned(768)
    for w in knz_sent:
        w.wait_recv()
    tot = knz[0]
    for k in range(1, NZ):
        tot = tot + knz[k]
    kna[...] = tot

    xb0 = x_back(0, zb0)
    xb1 = x_back(1, zb1)
    rl0 = x_relay(0, xb0)
    rl1 = x_relay(1, xb1)

    def finish(c, arrived):
        for w in arrived:
            w.wait_recv()
        cols = slice(c * CH, (c + 1) * CH)
        for i in range(2):
            a, b = split(full[c, i])
            mh[0:PROJ, i * CH:(i + 1) * CH] = a
            ml[0:PROJ, i * CH:(i + 1) * CH] = b
        mix = dot3(dh[...], dl[...], mh[0:PROJ, :], ml[0:PROJ, :])
        mr, mi = mix[:, :CH], mix[:, CH:]
        nonlocal_ = jnp.sum(full[c, 0] * mr + full[c, 1] * mi, axis=0, keepdims=True)
        for buf, (a, b) in zip((mh, ml), zip(split(mr), split(mi))):
            buf[0:PROJ, 0:CH] = a
            buf[0:PROJ, CH:2 * CH] = b
            buf[PROJ:2 * PROJ, 0:CH] = -b
            buf[PROJ:2 * PROJ, CH:2 * CH] = a
        kin, nrm = kna[2 * c:2 * c + 1, :], kna[2 * c + 1:2 * c + 2, :]
        est = (kin + nonlocal_) / (nrm + EPSILON)
        est_out[:, cols] = est
        energy = occ[:, cols] * nonlocal_ / (nrm + EPSILON)
        return est, energy

    def residual(c, est):
        cols = slice(c * CH, (c + 1) * CH)
        out = []
        for j, g in enumerate(range(0, GL, 256)):
            rows = slice(g, g + 256)
            acc = dot3(th[rows, :], tl[rows, :], mh[...], ml[...])
            shift = kcol[rows, :] - est
            rbuf[0, rows, cols] = shift * psi[0, rows, cols] + acc[:, :CH]
            rbuf[1, rows, cols] = shift * psi[1, rows, cols] + acc[:, CH:]
            copy = pltpu.make_async_copy(
                rbuf.at[:, rows, cols], res.at[:, rows, cols], out_sem.at[c, j]
            )
            copy.start()
            out.append(copy)
        return out

    est0, en0 = finish(0, xb0[2:] + rl0)
    outs = residual(0, est0)
    est1, en1 = finish(1, xb1[2:] + rl1)
    ebuf[band] = jnp.broadcast_to(en0 + en1, (8, CH))
    es = [remote(ebuf.at[band], ebuf.at[band], at_band(k)) for k in range(1, NBAND)]
    outs += residual(1, est1)
    for w in es:
        w.wait_recv()
    total = ebuf[0]
    for k in range(1, NBAND):
        total = total + ebuf[k]
    en_out[0, 0] = jnp.sum(total[0:1, :])
    for w in started:
        w.wait_send()
    for w in outs:
        w.wait()


NCOPY = NCH * (6 + 7 + 7 + 6) + 3 + 7 + 7


def on_device(waves, miller, positions, form_factors, coupling, species, block_sizes, occupation):
    vm = pl.BlockSpec(memory_space=pltpu.VMEM)
    res, est, en = pl.pallas_call(
        kernel,
        out_shape=(
            jax.ShapeDtypeStruct((2, GL, BL), F32),
            jax.ShapeDtypeStruct((1, BL), F32),
            jax.ShapeDtypeStruct((1, 1), F32),
        ),
        in_specs=[pl.BlockSpec(memory_space=pl.ANY)] + [vm] * 7,
        out_specs=(
            pl.BlockSpec(memory_space=pl.ANY),
            vm,
            pl.BlockSpec(memory_space=pltpu.SMEM),
        ),
        scratch_shapes=[
            pltpu.VMEM((2, GL, BL), F32),
            pltpu.VMEM((PROJ, 2 * GL), BF16),
            pltpu.VMEM((PROJ, 2 * GL), BF16),
            pltpu.VMEM((GL, 2 * PROJ), BF16),
            pltpu.VMEM((GL, 2 * PROJ), BF16),
            pltpu.VMEM((2 * GL, 2 * CH), BF16),
            pltpu.VMEM((2 * GL, 2 * CH), BF16),
            pltpu.VMEM((PROJ, PROJ), BF16),
            pltpu.VMEM((PROJ, PROJ), BF16),
            pltpu.VMEM((2 * PROJ, 2 * CH), BF16),
            pltpu.VMEM((2 * PROJ, 2 * CH), BF16),
            pltpu.VMEM((256, GL), BF16),
            pltpu.VMEM((128, GL), BF16),
            pltpu.VMEM((128, GL), BF16),
            pltpu.VMEM((256, 128), BF16),
            pltpu.VMEM((GL, CH), F32),
            pltpu.VMEM((NCH, 2, PROJ, CH), F32),
            pltpu.VMEM((NCH, 6, QR, CH), F32),
            pltpu.VMEM((NCH, 2, QR, CH), F32),
            pltpu.VMEM((NCH, 2, QR, CH), F32),
            pltpu.VMEM((NCH, NZ - 1, 2, SR, CH), F32),
            pltpu.VMEM((NCH, 2, PROJ, CH), F32),
            pltpu.VMEM((2, GL, BL), F32),
            pltpu.VMEM((NX, 8, CH), F32),
            pltpu.VMEM((NZ, 8, CH), F32),
            pltpu.VMEM((8, CH), F32),
            pltpu.VMEM((NBAND, 8, CH), F32),
            pltpu.SemaphoreType.DMA((2,)),
            pltpu.SemaphoreType.DMA((NCH, 4)),
            pltpu.SemaphoreType.DMA((NCOPY,)),
            pltpu.SemaphoreType.DMA((NCOPY,)),
        ],
        compiler_params=pltpu.CompilerParams(
            collective_id=0, has_side_effects=True, vmem_limit_bytes=60000 * 1024
        ),
    )(
        waves, miller, positions, form_factors, coupling,
        species.reshape(1, -1), block_sizes.reshape(1, -1), occupation.reshape(1, -1),
    )
    return res, est.reshape(BL), en.reshape(())


def solution(mesh):
    in_specs = (
        P(None, "ga", "band"),
        P(None, "ga"),
        P(),
        P(None, None, "ga"),
        P(),
        P(),
        P(),
        P("band"),
    )
    out_specs = (P(None, "ga", "band"), P("band"), P())
    return jax.shard_map(
        on_device, mesh=mesh, in_specs=in_specs, out_specs=out_specs, check_vma=False
    )
```

```python
import jax
import jax.numpy as jnp
from jax import lax
from jax.experimental import pallas as pl
from jax.experimental.pallas import tpu as pltpu
from jax.sharding import PartitionSpec as P

MESH = pl.DeviceIdType.MESH
F32 = jnp.float32
BF16 = jnp.bfloat16

NX = 4
NZ = 8
NBAND = 8
PROJ = 512
ATOMS = 64
NSPEC = 4
KMAX = 18
GL = 1024
BL = 256
CH = 128
NCH = BL // CH
QR = PROJ // NX
SR = QR // NZ

FAR_FIRST = (4, 3, 5, 2, 6, 1, 7)
NEAR_FIRST = (1, 7, 2, 6, 3, 5, 4)

KINETIC_SCALE = 0.005
EPSILON = 1e-6

SIN_C = (3.141592653589793, -5.16771278004997, 2.550164039877345, -0.5992645293207921, 0.08214588661112823, -0.00737043094571435, 0.00046630280576761255)
COS_C = (1.0, -4.934802200544679, 4.058712126416768, -1.3352627688545893, 0.2353306303588935, -0.02580689139001406, 0.0019295743094039231)


def split(x):
    hi = x.astype(BF16)
    return hi, (x - hi.astype(F32)).astype(BF16)


def dot(a, b):
    return jnp.dot(a, b, preferred_element_type=F32)


def dot3(ah, al, bh, bl):
    return dot(ah, bh) + dot(al, bh) + dot(ah, bl)


def horner(coeffs, x):
    acc = jnp.full_like(x, coeffs[-1])
    for c in coeffs[-2::-1]:
        acc = acc * x + c
    return acc


def iota(shape, dim):
    return lax.broadcasted_iota(jnp.int32, shape, dim)


def kernel(waves, miller, pos, ff, coup, spec, size, occ,
           res, est_out, en_out,
           psi, bh, bl, th, tl, vh, vl, dh, dl, mh, ml,
           ffs, ffk, ctk, stk, cks, ckk, kcol, pbuf, xr, q, zr, full, rbuf,
           knx, knz, kna, ebuf,
           in_sem, out_sem, send, recv):
    gi = lax.axis_index("ga")
    band = lax.axis_index("band")
    z = lax.div(gi, NX)
    x = lax.rem(gi, NX)
    r, o, l = (lax.rem(x + k, NX) for k in (1, 2, 3))

    def at_x(xx):
        return {"ga": z * NX + xx}

    def at_z(k):
        return {"ga": lax.rem(z + k, NZ) * NX + x}

    def at_band(k):
        return {"band": lax.rem(band + k, NBAND)}

    loads = [pltpu.make_async_copy(waves.at[i], psi.at[i], in_sem.at[i]) for i in range(2)]
    for c in loads:
        c.start()

    barrier = pltpu.get_barrier_semaphore()
    peers = [at_x(r), at_x(l), at_x(o)] + [at_z(k) for k in range(1, NZ)] + [at_band(k) for k in range(1, NBAND)]
    for p in peers:
        pl.semaphore_signal(barrier, inc=1, device_id=p, device_id_type=MESH)

    started = []
    slot = [0]

    def remote(src, dst, where):
        i = slot[0]
        slot[0] += 1
        copy = pltpu.make_async_remote_copy(
            src_ref=src, dst_ref=dst, send_sem=send.at[i], recv_sem=recv.at[i],
            device_id=where, device_id_type=MESH,
        )
        started.append(copy)
        copy.start()
        return copy

    size_row = size[...].astype(F32)
    spec_row = spec[...].astype(F32)
    i0, i1 = iota((ATOMS, ATOMS), 0), iota((ATOMS, ATOMS), 1)
    size_col = jnp.sum(jnp.where(i0 == i1, size_row, 0.0), axis=1, keepdims=True)
    end_row = jnp.sum(jnp.where(i0 <= i1, size_col, 0.0), axis=0, keepdims=True)
    end_col = jnp.sum(jnp.where(i1 <= i0, size_row, 0.0), axis=1, keepdims=True)
    start_row = end_row - size_row
    start_col = end_col - size_col
    p_col = iota((PROJ, ATOMS), 0).astype(F32)
    own = (p_col >= start_row) & (p_col < end_row)
    atom_row = iota((1, ATOMS), 1).astype(F32)
    owner_col = jnp.sum(jnp.where(own, atom_row, 0.0), axis=1, keepdims=True)
    row_col = jnp.sum(jnp.where(own, spec_row + NSPEC * (p_col - start_row), 0.0), axis=1, keepdims=True)
    lane = iota((PROJ, 256), 1)
    row_hot = jnp.where(lax.rem(lane, 128).astype(F32) == row_col, 1.0, 0.0).astype(BF16)
    own_hot = jnp.where(lax.rem(lane[:, :128], 64).astype(F32) == owner_col, 1.0, 0.0).astype(BF16)

    ffs[72:80, :] = jnp.zeros((8, GL), F32)
    for k in range(KMAX):
        ffs[k * NSPEC:(k + 1) * NSPEC, :] = ff[k]
    for g in range(0, 256, 128):
        ffk[g + 80:g + 128, :] = jnp.zeros((48, GL), BF16)
    ffk[0:80, :], ffk[128:208, :] = split(ffs[...])
    pos_col = [
        jnp.sum(jnp.where(i0 == i1, pos[i:i + 1, :], 0.0), axis=1, keepdims=True) for i in range(3)
    ]
    m = miller[...].astype(F32)
    for g in range(0, GL, 256):
        mg = m[:, g:g + 256]
        turns = pos_col[0] * mg[0:1] + pos_col[1] * mg[1:2] + pos_col[2] * mg[2:3]
        turns = turns - jnp.round(turns)
        t2 = turns * turns
        sh = horner(SIN_C, t2) * turns
        ch = horner(COS_C, t2)
        for dst, val in ((ctk, 1.0 - 2.0 * (sh * sh)), (stk, 2.0 * (sh * ch))):
            a, b = split(val)
            dst[0:64, g:g + 256] = a
            dst[64:128, g:g + 256] = b
        radial = dot(row_hot, ffk[:, g:g + 256])
        for base, tab, sign in ((0, ctk, 1.0), (GL, stk, -1.0)):
            b = radial * dot(own_hot, tab[:, g:g + 256])
            b = b if sign > 0 else -b
            a, b = split(b)
            bh[:, base + g:base + g + 256] = a
            bl[:, base + g:base + g + 256] = b
    ksum = m[0:1] * m[0:1] + m[1:2] * m[1:2] + m[2:3] * m[2:3]
    krow = jnp.broadcast_to(0.5 * KINETIC_SCALE * ksum, (128, GL))
    for g in range(0, GL, 128):
        kcol[g:g + 128, :] = jnp.transpose(krow[:, g:g + 128])

    for c in loads:
        c.wait()

    def project(c):
        cols = slice(c * CH, (c + 1) * CH)
        rows = 256
        kin = jnp.zeros((1, CH), F32)
        nrm = jnp.zeros((1, CH), F32)
        for g in range(0, GL, rows):
            pr = psi[0, g:g + rows, cols]
            pi = psi[1, g:g + rows, cols]
            den = pr * pr + pi * pi
            nrm = nrm + jnp.sum(den, axis=0, keepdims=True)
            kin = kin + jnp.sum(kcol[g:g + rows, :] * den, axis=0, keepdims=True)
            for buf, (a, b) in zip((vh, vl), zip(split(pr), split(pi))):
                buf[g:g + rows, 0:CH] = a
                buf[g:g + rows, CH:2 * CH] = b
                buf[GL + g:GL + g + rows, 0:CH] = b
                buf[GL + g:GL + g + rows, CH:2 * CH] = -a
        p = dot3(bh[...], bl[...], vh[...], vl[...])
        pbuf[c, 0] = p[:, :CH]
        pbuf[c, 1] = p[:, CH:]
        return kin, nrm

    def rows_of(xx, zz):
        return pl.ds(pl.multiple_of(xx * QR + zz * SR, SR), SR)

    def z_at(k):
        return lax.rem(z + k, NZ)

    def x_at(k):
        return lax.rem(x + k, NX)

    def x_first(c):
        return {
            (k, d): remote(pbuf.at[c, :, rows_of(x_at(d), z_at(k)), :], xr.at[c, k, d - 1], at_x(x_at(d)))
            for k in FAR_FIRST + (0,)
            for d in (2, 1, 3)
        }

    def z_first(c, xs):
        out = {}
        for k in FAR_FIRST + (0,):
            for d in (2, 1, 3):
                xs[k, d].wait_recv()
            q[c, k] = pbuf[c, :, rows_of(x, z_at(k)), :] + xr[c, k, 0] + xr[c, k, 1] + xr[c, k, 2]
            if k:
                out[k] = remote(q.at[c, k], zr.at[c, k - 1], at_z(k))
        return out

    mine = rows_of(x, z)

    def spread(c, zz):
        part = full.at[c, :, rows_of(x, zz), :]
        return [remote(part, part, at_x(x_at(d))) for d in (2, 1, 3)]

    def z_back(c, zs):
        for k in FAR_FIRST:
            zs[k].wait_recv()
        share = q[c, 0]
        for k in range(NZ - 1):
            share = share + zr[c, k]
        full[c, :, mine, :] = share
        part = full.at[c, :, mine, :]
        back = {k: remote(part, part, at_z(k)) for k in NEAR_FIRST}
        return back, spread(c, z)

    def x_back(c, back):
        out = []
        for k in NEAR_FIRST:
            back[k].wait_recv()
            out += spread(c, z_at(NZ - k))
        return out

    kn0 = project(0)
    pl.semaphore_wait(barrier, len(peers))
    first0 = x_first(0)
    kn1 = project(1)
    first1 = x_first(1)

    tile_row = iota((8, CH), 0)
    kn = jnp.zeros((8, CH), F32)
    for i, v in enumerate((kn0[0], kn0[1], kn1[0], kn1[1])):
        kn = jnp.where(tile_row == i, v, kn)
    knx[x] = kn
    knx_sent = [remote(knx.at[x], knx.at[x], at_x(k)) for k in (r, l, o)]

    zs0 = z_first(0, first0)

    for w in knx_sent:
        w.wait_recv()
    knz[z] = knx[0] + knx[1] + knx[2] + knx[3]
    knz_sent = [remote(knz.at[z], knz.at[z], at_z(k)) for k in range(1, NZ)]

    cks[...] = jnp.zeros_like(cks)
    for k in range(KMAX):
        cks[k * NSPEC:(k + 1) * NSPEC, 0:KMAX] = coup[k]
    ckk[0:128, :], ckk[128:256, :] = split(cks[...])
    q_row = iota((ATOMS, PROJ), 1).astype(F32)
    own_t = (q_row >= start_col) & (q_row < end_col)
    atom_col = iota((ATOMS, 1), 0).astype(F32)
    owner_row = jnp.sum(jnp.where(own_t, atom_col, 0.0), axis=0, keepdims=True)
    chan_row = jnp.sum(jnp.where(own_t, q_row - start_col, 0.0), axis=0, keepdims=True)
    chan_hot = jnp.where(iota((128, PROJ), 0).astype(F32) == chan_row, 1.0, 0.0).astype(BF16)
    same = owner_col == owner_row
    for dst, part in ((dh, row_hot[:, :128]), (dl, row_hot[:, 128:])):
        base = 0 if dst is dh else 128
        table = dot(part, ckk[base:base + 128, :]).astype(BF16)
        dst[...] = jnp.where(same, dot(table, chan_hot), 0.0).astype(BF16)

    zs1 = z_first(1, first1)

    def turned(g):
        for src, dst in ((bh, th), (bl, tl)):
            for half in range(2):
                dst[g:g + 256, half * PROJ:(half + 1) * PROJ] = jnp.transpose(
                    src[:, half * GL + g:half * GL + g + 256]
                )

    turned(0)
    back0, sp0 = z_back(0, zs0)
    turned(256)
    sp0 += x_back(0, back0)
    back1, sp1 = z_back(1, zs1)
    turned(512)
    turned(768)
    for w in knz_sent:
        w.wait_recv()
    tot = knz[0]
    for k in range(1, NZ):
        tot = tot + knz[k]
    kna[...] = tot
    sp1 += x_back(1, back1)

    def finish(c, arrived):
        for w in arrived:
            w.wait_recv()
        cols = slice(c * CH, (c + 1) * CH)
        for i in range(2):
            a, b = split(full[c, i])
            mh[0:PROJ, i * CH:(i + 1) * CH] = a
            ml[0:PROJ, i * CH:(i + 1) * CH] = b
        mix = dot3(dh[...], dl[...], mh[0:PROJ, :], ml[0:PROJ, :])
        mr, mi = mix[:, :CH], mix[:, CH:]
        nonlocal_ = jnp.sum(full[c, 0] * mr + full[c, 1] * mi, axis=0, keepdims=True)
        for buf, (a, b) in zip((mh, ml), zip(split(mr), split(mi))):
            buf[0:PROJ, 0:CH] = a
            buf[0:PROJ, CH:2 * CH] = b
            buf[PROJ:2 * PROJ, 0:CH] = -b
            buf[PROJ:2 * PROJ, CH:2 * CH] = a
        kin, nrm = kna[2 * c:2 * c + 1, :], kna[2 * c + 1:2 * c + 2, :]
        est = (kin + nonlocal_) / (nrm + EPSILON)
        est_out[:, cols] = est
        energy = occ[:, cols] * nonlocal_ / (nrm + EPSILON)
        return est, energy

    def residual(c, est):
        cols = slice(c * CH, (c + 1) * CH)
        out = []
        for j, g in enumerate(range(0, GL, 256)):
            rows = slice(g, g + 256)
            acc = dot3(th[rows, :], tl[rows, :], mh[...], ml[...])
            shift = kcol[rows, :] - est
            rbuf[0, rows, cols] = shift * psi[0, rows, cols] + acc[:, :CH]
            rbuf[1, rows, cols] = shift * psi[1, rows, cols] + acc[:, CH:]
            copy = pltpu.make_async_copy(
                rbuf.at[:, rows, cols], res.at[:, rows, cols], out_sem.at[c, j]
            )
            copy.start()
            out.append(copy)
        return out

    est0, en0 = finish(0, sp0)
    outs = residual(0, est0)
    est1, en1 = finish(1, sp1)
    ebuf[band] = jnp.broadcast_to(en0 + en1, (8, CH))
    es = [remote(ebuf.at[band], ebuf.at[band], at_band(k)) for k in range(1, NBAND)]
    outs += residual(1, est1)
    for w in es:
        w.wait_recv()
    total = ebuf[0]
    for k in range(1, NBAND):
        total = total + ebuf[k]
    en_out[0, 0] = jnp.sum(total[0:1, :])
    for w in started:
        w.wait_send()
    for w in outs:
        w.wait()


NCOPY = NCH * (24 + 7 + 7 + 24) + 3 + 7 + 7


def on_device(waves, miller, positions, form_factors, coupling, species, block_sizes, occupation):
    vm = pl.BlockSpec(memory_space=pltpu.VMEM)
    res, est, en = pl.pallas_call(
        kernel,
        out_shape=(
            jax.ShapeDtypeStruct((2, GL, BL), F32),
            jax.ShapeDtypeStruct((1, BL), F32),
            jax.ShapeDtypeStruct((1, 1), F32),
        ),
        in_specs=[pl.BlockSpec(memory_space=pl.ANY)] + [vm] * 7,
        out_specs=(
            pl.BlockSpec(memory_space=pl.ANY),
            vm,
            pl.BlockSpec(memory_space=pltpu.SMEM),
        ),
        scratch_shapes=[
            pltpu.VMEM((2, GL, BL), F32),
            pltpu.VMEM((PROJ, 2 * GL), BF16),
            pltpu.VMEM((PROJ, 2 * GL), BF16),
            pltpu.VMEM((GL, 2 * PROJ), BF16),
            pltpu.VMEM((GL, 2 * PROJ), BF16),
            pltpu.VMEM((2 * GL, 2 * CH), BF16),
            pltpu.VMEM((2 * GL, 2 * CH), BF16),
            pltpu.VMEM((PROJ, PROJ), BF16),
            pltpu.VMEM((PROJ, PROJ), BF16),
            pltpu.VMEM((2 * PROJ, 2 * CH), BF16),
            pltpu.VMEM((2 * PROJ, 2 * CH), BF16),
            pltpu.VMEM((80, GL), F32),
            pltpu.VMEM((256, GL), BF16),
            pltpu.VMEM((128, GL), BF16),
            pltpu.VMEM((128, GL), BF16),
            pltpu.VMEM((128, 128), F32),
            pltpu.VMEM((256, 128), BF16),
            pltpu.VMEM((GL, CH), F32),
            pltpu.VMEM((NCH, 2, PROJ, CH), F32),
            pltpu.VMEM((NCH, NZ, NX - 1, 2, SR, CH), F32),
            pltpu.VMEM((NCH, NZ, 2, SR, CH), F32),
            pltpu.VMEM((NCH, NZ - 1, 2, SR, CH), F32),
            pltpu.VMEM((NCH, 2, PROJ, CH), F32),
            pltpu.VMEM((2, GL, BL), F32),
            pltpu.VMEM((NX, 8, CH), F32),
            pltpu.VMEM((NZ, 8, CH), F32),
            pltpu.VMEM((8, CH), F32),
            pltpu.VMEM((NBAND, 8, CH), F32),
            pltpu.SemaphoreType.DMA((2,)),
            pltpu.SemaphoreType.DMA((NCH, 4)),
            pltpu.SemaphoreType.DMA((NCOPY,)),
            pltpu.SemaphoreType.DMA((NCOPY,)),
        ],
        compiler_params=pltpu.CompilerParams(
            collective_id=0, has_side_effects=True, vmem_limit_bytes=60000 * 1024
        ),
    )(
        waves, miller, positions.T, form_factors.transpose(1, 0, 2), coupling.transpose(1, 0, 2),
        species.reshape(1, -1), block_sizes.reshape(1, -1), occupation.reshape(1, -1),
    )
    return res, est.reshape(BL), en.reshape(())


def solution(mesh):
    in_specs = (
        P(None, "ga", "band"),
        P(None, "ga"),
        P(),
        P(None, None, "ga"),
        P(),
        P(),
        P(),
        P("band"),
    )
    out_specs = (P(None, "ga", "band"), P("band"), P())
    return jax.shard_map(
        on_device, mesh=mesh, in_specs=in_specs, out_specs=out_specs, check_vma=False
    )
```

```python
import jax
import jax.numpy as jnp
from jax import lax
from jax.experimental import pallas as pl
from jax.experimental.pallas import tpu as pltpu
from jax.sharding import PartitionSpec as P

MESH = pl.DeviceIdType.MESH
F32 = jnp.float32
BF16 = jnp.bfloat16

NX = 4
NZ = 8
NBAND = 8
PROJ = 512
ATOMS = 64
NSPEC = 4
KMAX = 18
GL = 1024
BL = 256
CH = 128
NCH = BL // CH
QR = PROJ // NX
SR = QR // NZ

FAR_FIRST = (4, 3, 5, 2, 6, 1, 7)
NEAR_FIRST = (1, 7, 2, 6, 3, 5, 4)

KINETIC_SCALE = 0.005
EPSILON = 1e-6

SIN_C = (3.141592653589793, -5.16771278004997, 2.550164039877345, -0.5992645293207921, 0.08214588661112823, -0.00737043094571435, 0.00046630280576761255)
COS_C = (1.0, -4.934802200544679, 4.058712126416768, -1.3352627688545893, 0.2353306303588935, -0.02580689139001406, 0.0019295743094039231)


def split(x):
    hi = x.astype(BF16)
    return hi, (x - hi.astype(F32)).astype(BF16)


def dot(a, b):
    return jnp.dot(a, b, preferred_element_type=F32)


def dot3(ah, al, bh, bl):
    return dot(ah, bh) + dot(al, bh) + dot(ah, bl)


def horner(coeffs, x):
    acc = jnp.full_like(x, coeffs[-1])
    for c in coeffs[-2::-1]:
        acc = acc * x + c
    return acc


def iota(shape, dim):
    return lax.broadcasted_iota(jnp.int32, shape, dim)


def kernel(waves, miller_in, pos_in, ff_in, coup_in, spec_in, size_in, occ_in,
           res, est_to, en_out,
           psi, bh, bl, th, tl, vh, vl, dh, dl, mh, ml,
           ffs, ffk, ctk, stk, cks, ckk, kcol, pbuf, xr, q, zr, full, rbuf,
           knx, knz, kna, ebuf, miller, pos, ff, coup, spec, size, occ, est_out,
           in_sem, est_sem, out_sem, sent, xr_sem, zr_sem, za_sem, xa_sem, kn_sem):
    gi = lax.axis_index("ga")
    band = lax.axis_index("band")
    z = lax.div(gi, NX)
    x = lax.rem(gi, NX)
    r, o, l = (lax.rem(x + k, NX) for k in (1, 2, 3))

    def at_x(xx):
        return {"ga": z * NX + xx}

    def at_z(k):
        return {"ga": lax.rem(z + k, NZ) * NX + x}

    def at_band(k):
        return {"band": lax.rem(band + k, NBAND)}

    smalls = [
        pltpu.make_async_copy(a, b, in_sem.at[2 + i])
        for i, (a, b) in enumerate((
            (size_in, size), (spec_in, spec), (pos_in, pos), (miller_in, miller),
            (ff_in, ff), (coup_in, coup), (occ_in, occ),
        ))
    ]
    loads = [pltpu.make_async_copy(waves.at[i], psi.at[i], in_sem.at[i]) for i in range(2)]
    for c in smalls + loads:
        c.start()

    barrier = pltpu.get_barrier_semaphore()
    peers = [at_x(r), at_x(l), at_x(o)] + [at_z(k) for k in range(1, NZ)] + [at_band(k) for k in range(1, NBAND)]
    for p in peers:
        pl.semaphore_signal(barrier, inc=1, device_id=p, device_id_type=MESH)

    def remote(src, dst, where, recv_sem, send_sem=None):
        copy = pltpu.make_async_remote_copy(
            src_ref=src, dst_ref=dst, send_sem=sent.at[0] if send_sem is None else send_sem,
            recv_sem=recv_sem, device_id=where, device_id_type=MESH,
        )
        copy.start()
        return copy

    def arrived(ref, sem):
        pltpu.make_async_copy(ref, ref, sem).wait()

    for c in smalls:
        c.wait()
    size_row = size[...].astype(F32)
    spec_row = spec[...].astype(F32)
    i0, i1 = iota((ATOMS, ATOMS), 0), iota((ATOMS, ATOMS), 1)
    size_col = jnp.sum(jnp.where(i0 == i1, size_row, 0.0), axis=1, keepdims=True)
    end_row = jnp.sum(jnp.where(i0 <= i1, size_col, 0.0), axis=0, keepdims=True)
    end_col = jnp.sum(jnp.where(i1 <= i0, size_row, 0.0), axis=1, keepdims=True)
    start_row = end_row - size_row
    start_col = end_col - size_col
    p_col = iota((PROJ, ATOMS), 0).astype(F32)
    own = (p_col >= start_row) & (p_col < end_row)
    atom_row = iota((1, ATOMS), 1).astype(F32)
    owner_col = jnp.sum(jnp.where(own, atom_row, 0.0), axis=1, keepdims=True)
    row_col = jnp.sum(jnp.where(own, spec_row + NSPEC * (p_col - start_row), 0.0), axis=1, keepdims=True)
    lane = iota((PROJ, 256), 1)
    row_hot = jnp.where((lane & 127).astype(F32) == row_col, 1.0, 0.0).astype(BF16)
    own_hot = jnp.where((lane[:, :128] & 63).astype(F32) == owner_col, 1.0, 0.0).astype(BF16)

    ffs[72:80, :] = jnp.zeros((8, GL), F32)
    for k in range(KMAX):
        ffs[k * NSPEC:(k + 1) * NSPEC, :] = ff[k]
    for g in range(0, 256, 128):
        ffk[g + 80:g + 128, :] = jnp.zeros((48, GL), BF16)
    ffk[0:80, :], ffk[128:208, :] = split(ffs[...])
    pos_col = [
        jnp.sum(jnp.where(i0 == i1, pos[i:i + 1, :], 0.0), axis=1, keepdims=True) for i in range(3)
    ]
    m = miller[...].astype(F32)
    for g in range(0, GL, 256):
        mg = m[:, g:g + 256]
        turns = pos_col[0] * mg[0:1] + pos_col[1] * mg[1:2] + pos_col[2] * mg[2:3]
        turns = turns - jnp.round(turns)
        t2 = turns * turns
        sh = horner(SIN_C, t2) * turns
        ch = horner(COS_C, t2)
        for dst, val in ((ctk, 1.0 - 2.0 * (sh * sh)), (stk, 2.0 * (sh * ch))):
            a, b = split(val)
            dst[0:64, g:g + 256] = a
            dst[64:128, g:g + 256] = b
        radial = dot(row_hot, ffk[:, g:g + 256])
        for base, tab, sign in ((0, ctk, 1.0), (GL, stk, -1.0)):
            b = radial * dot(own_hot, tab[:, g:g + 256])
            b = b if sign > 0 else -b
            a, b = split(b)
            bh[:, base + g:base + g + 256] = a
            bl[:, base + g:base + g + 256] = b
    ksum = m[0:1] * m[0:1] + m[1:2] * m[1:2] + m[2:3] * m[2:3]
    krow = jnp.broadcast_to(0.5 * KINETIC_SCALE * ksum, (128, GL))
    for g in range(0, GL, 128):
        kcol[g:g + 128, :] = jnp.transpose(krow[:, g:g + 128])

    for c in loads:
        c.wait()

    def project(c):
        cols = slice(c * CH, (c + 1) * CH)
        rows = 256
        kin = jnp.zeros((1, CH), F32)
        nrm = jnp.zeros((1, CH), F32)
        for g in range(0, GL, rows):
            pr = psi[0, g:g + rows, cols]
            pi = psi[1, g:g + rows, cols]
            den = pr * pr + pi * pi
            nrm = nrm + jnp.sum(den, axis=0, keepdims=True)
            kin = kin + jnp.sum(kcol[g:g + rows, :] * den, axis=0, keepdims=True)
            for buf, (a, b) in zip((vh, vl), zip(split(pr), split(pi))):
                buf[g:g + rows, 0:CH] = a
                buf[g:g + rows, CH:2 * CH] = b
                buf[GL + g:GL + g + rows, 0:CH] = b
                buf[GL + g:GL + g + rows, CH:2 * CH] = -a
        p = dot3(bh[...], bl[...], vh[...], vl[...])
        pbuf[c, 0] = p[:, :CH]
        pbuf[c, 1] = p[:, CH:]
        return kin, nrm

    def rows_of(xx, zz):
        return pl.ds(pl.multiple_of(xx * QR + zz * SR, SR), SR)

    def z_at(k):
        return lax.rem(z + k, NZ)

    def x_at(k):
        return lax.rem(x + k, NX)

    def x_first(c):
        for k in FAR_FIRST + (0,):
            for d in (2, 1, 3):
                part = pbuf.at[c, :, rows_of(x_at(d), z_at(k)), :]
                remote(part, xr.at[c, k, d - 1], at_x(x_at(d)), xr_sem.at[c, k])

    def z_first(c):
        for k in FAR_FIRST + (0,):
            arrived(xr.at[c, k], xr_sem.at[c, k])
            q[c, k] = pbuf[c, :, rows_of(x, z_at(k)), :] + xr[c, k, 0] + xr[c, k, 1] + xr[c, k, 2]
            if k:
                remote(q.at[c, k], zr.at[c, k - 1], at_z(k), zr_sem.at[c])

    mine = rows_of(x, z)

    def spread(c, zz):
        part = full.at[c, :, rows_of(x, zz), :]
        for d in (2, 1, 3):
            remote(part, part, at_x(x_at(d)), xa_sem.at[c])

    def z_back(c):
        arrived(zr.at[c], zr_sem.at[c])
        share = q[c, 0]
        for k in range(NZ - 1):
            share = share + zr[c, k]
        full[c, :, mine, :] = share
        part = full.at[c, :, mine, :]
        spread(c, z)
        return {k: remote(part, part, at_z(k), za_sem.at[c, k - 1]) for k in NEAR_FIRST}

    def x_back(c, back):
        for k in NEAR_FIRST:
            back[k].wait_recv()
            spread(c, z_at(NZ - k))

    kn0 = project(0)
    pl.semaphore_wait(barrier, len(peers))
    x_first(0)
    kn1 = project(1)
    x_first(1)

    tile_row = iota((8, CH), 0)
    kn = jnp.zeros((8, CH), F32)
    for i, v in enumerate((kn0[0], kn0[1], kn1[0], kn1[1])):
        kn = jnp.where(tile_row == i, v, kn)
    knx[x] = kn
    for k in (r, l, o):
        remote(knx.at[x], knx.at[x], at_x(k), kn_sem.at[0], sent.at[1])

    z_first(0)

    arrived(knx.at[0:NX - 1], kn_sem.at[0])
    knz[z] = knx[0] + knx[1] + knx[2] + knx[3]
    for k in range(1, NZ):
        remote(knz.at[z], knz.at[z], at_z(k), kn_sem.at[1], sent.at[1])

    cks[...] = jnp.zeros_like(cks)
    for k in range(KMAX):
        cks[k * NSPEC:(k + 1) * NSPEC, 0:KMAX] = coup[k]
    ckk[0:128, :], ckk[128:256, :] = split(cks[...])
    q_row = iota((ATOMS, PROJ), 1).astype(F32)
    own_t = (q_row >= start_col) & (q_row < end_col)
    atom_col = iota((ATOMS, 1), 0).astype(F32)
    owner_row = jnp.sum(jnp.where(own_t, atom_col, 0.0), axis=0, keepdims=True)
    chan_row = jnp.sum(jnp.where(own_t, q_row - start_col, 0.0), axis=0, keepdims=True)
    chan_hot = jnp.where(iota((128, PROJ), 0).astype(F32) == chan_row, 1.0, 0.0).astype(BF16)
    same = owner_col == owner_row
    for dst, part in ((dh, row_hot[:, :128]), (dl, row_hot[:, 128:])):
        base = 0 if dst is dh else 128
        table = dot(part, ckk[base:base + 128, :]).astype(BF16)
        dst[...] = jnp.where(same, dot(table, chan_hot), 0.0).astype(BF16)

    z_first(1)

    def turned(g):
        for src, dst in ((bh, th), (bl, tl)):
            for half in range(2):
                dst[g:g + 256, half * PROJ:(half + 1) * PROJ] = jnp.transpose(
                    src[:, half * GL + g:half * GL + g + 256]
                )

    turned(0)
    back0 = z_back(0)
    turned(256)
    x_back(0, back0)
    back1 = z_back(1)
    turned(512)
    turned(768)
    arrived(knz.at[0:NZ - 1], kn_sem.at[1])
    tot = knz[0]
    for k in range(1, NZ):
        tot = tot + knz[k]
    kna[...] = tot
    x_back(1, back1)

    def finish(c):
        arrived(full.at[c, :, 0:PROJ - QR, :], xa_sem.at[c])
        cols = slice(c * CH, (c + 1) * CH)
        for i in range(2):
            a, b = split(full[c, i])
            mh[0:PROJ, i * CH:(i + 1) * CH] = a
            ml[0:PROJ, i * CH:(i + 1) * CH] = b
        mix = dot3(dh[...], dl[...], mh[0:PROJ, :], ml[0:PROJ, :])
        mr, mi = mix[:, :CH], mix[:, CH:]
        nonlocal_ = jnp.sum(full[c, 0] * mr + full[c, 1] * mi, axis=0, keepdims=True)
        for buf, (a, b) in zip((mh, ml), zip(split(mr), split(mi))):
            buf[0:PROJ, 0:CH] = a
            buf[0:PROJ, CH:2 * CH] = b
            buf[PROJ:2 * PROJ, 0:CH] = -b
            buf[PROJ:2 * PROJ, CH:2 * CH] = a
        kin, nrm = kna[2 * c:2 * c + 1, :], kna[2 * c + 1:2 * c + 2, :]
        est = (kin + nonlocal_) / (nrm + EPSILON)
        est_out[:, cols] = est
        energy = occ[:, cols] * nonlocal_ / (nrm + EPSILON)
        return est, energy

    def residual(c, est):
        cols = slice(c * CH, (c + 1) * CH)
        out = []
        acc = dot3(th[...], tl[...], mh[...], ml[...])
        for i in range(2):
            rbuf[i, :, cols] = (kcol[...] - est) * psi[i, :, cols] + acc[:, i * CH:(i + 1) * CH]
            copy = pltpu.make_async_copy(rbuf.at[i, :, cols], res.at[i, :, cols], out_sem.at[c, i])
            copy.start()
            out.append(copy)
        return out

    est0, en0 = finish(0)
    outs = residual(0, est0)
    est1, en1 = finish(1)
    ebuf[band] = jnp.broadcast_to(en0 + en1, (8, CH))
    for k in range(1, NBAND):
        remote(ebuf.at[band], ebuf.at[band], at_band(k), kn_sem.at[2], sent.at[1])
    est_copy = pltpu.make_async_copy(est_out, est_to, est_sem)
    est_copy.start()
    outs += residual(1, est1) + [est_copy]
    arrived(ebuf.at[0:NBAND - 1], kn_sem.at[2])
    total = ebuf[0]
    for k in range(1, NBAND):
        total = total + ebuf[k]
    en_out[0, 0] = jnp.sum(total[0:1, :])
    arrived(rbuf.at[:, 0:NPIECE * 8, :], sent.at[0])
    arrived(pbuf.at[0, 0, 0:NTILE * 8, :], sent.at[1])
    for w in outs:
        w.wait()


NPIECE = NCH * (24 + 7 + 7 + 24)
NTILE = 3 + 7 + 7


def on_device(waves, miller, positions, form_factors, coupling, species, block_sizes, occupation):
    anywhere = pl.BlockSpec(memory_space=pl.ANY)
    res, est, en = pl.pallas_call(
        kernel,
        out_shape=(
            jax.ShapeDtypeStruct((2, GL, BL), F32),
            jax.ShapeDtypeStruct((1, BL), F32),
            jax.ShapeDtypeStruct((1, 1), F32),
        ),
        in_specs=[anywhere] * 8,
        out_specs=(
            anywhere,
            anywhere,
            pl.BlockSpec(memory_space=pltpu.SMEM),
        ),
        scratch_shapes=[
            pltpu.VMEM((2, GL, BL), F32),
            pltpu.VMEM((PROJ, 2 * GL), BF16),
            pltpu.VMEM((PROJ, 2 * GL), BF16),
            pltpu.VMEM((GL, 2 * PROJ), BF16),
            pltpu.VMEM((GL, 2 * PROJ), BF16),
            pltpu.VMEM((2 * GL, 2 * CH), BF16),
            pltpu.VMEM((2 * GL, 2 * CH), BF16),
            pltpu.VMEM((PROJ, PROJ), BF16),
            pltpu.VMEM((PROJ, PROJ), BF16),
            pltpu.VMEM((2 * PROJ, 2 * CH), BF16),
            pltpu.VMEM((2 * PROJ, 2 * CH), BF16),
            pltpu.VMEM((80, GL), F32),
            pltpu.VMEM((256, GL), BF16),
            pltpu.VMEM((128, GL), BF16),
            pltpu.VMEM((128, GL), BF16),
            pltpu.VMEM((128, 128), F32),
            pltpu.VMEM((256, 128), BF16),
            pltpu.VMEM((GL, CH), F32),
            pltpu.VMEM((NCH, 2, PROJ, CH), F32),
            pltpu.VMEM((NCH, NZ, NX - 1, 2, SR, CH), F32),
            pltpu.VMEM((NCH, NZ, 2, SR, CH), F32),
            pltpu.VMEM((NCH, NZ - 1, 2, SR, CH), F32),
            pltpu.VMEM((NCH, 2, PROJ, CH), F32),
            pltpu.VMEM((2, GL, BL), F32),
            pltpu.VMEM((NX, 8, CH), F32),
            pltpu.VMEM((NZ, 8, CH), F32),
            pltpu.VMEM((8, CH), F32),
            pltpu.VMEM((NBAND, 8, CH), F32),
            pltpu.VMEM((3, GL), jnp.int32),
            pltpu.VMEM((3, ATOMS), F32),
            pltpu.VMEM((KMAX, NSPEC, GL), F32),
            pltpu.VMEM((KMAX, NSPEC, KMAX), F32),
            pltpu.VMEM((1, ATOMS), jnp.int32),
            pltpu.VMEM((1, ATOMS), jnp.int32),
            pltpu.VMEM((1, BL), F32),
            pltpu.VMEM((1, BL), F32),
            pltpu.SemaphoreType.DMA((9,)),
            pltpu.SemaphoreType.DMA,
            pltpu.SemaphoreType.DMA((NCH, 2)),
            pltpu.SemaphoreType.DMA((2,)),
            pltpu.SemaphoreType.DMA((NCH, NZ)),
            pltpu.SemaphoreType.DMA((NCH,)),
            pltpu.SemaphoreType.DMA((NCH, NZ - 1)),
            pltpu.SemaphoreType.DMA((NCH,)),
            pltpu.SemaphoreType.DMA((3,)),
        ],
        compiler_params=pltpu.CompilerParams(
            collective_id=0, has_side_effects=True, vmem_limit_bytes=60000 * 1024
        ),
    )(
        waves, miller, positions.T, form_factors.transpose(1, 0, 2), coupling.transpose(1, 0, 2),
        species.reshape(1, -1), block_sizes.reshape(1, -1), occupation.reshape(1, -1),
    )
    return res, est.reshape(BL), en.reshape(())


def solution(mesh):
    in_specs = (
        P(None, "ga", "band"),
        P(None, "ga"),
        P(),
        P(None, None, "ga"),
        P(),
        P(),
        P(),
        P("band"),
    )
    out_specs = (P(None, "ga", "band"), P("band"), P())
    return jax.shard_map(
        on_device, mesh=mesh, in_specs=in_specs, out_specs=out_specs, check_vma=False
    )
```

```python
import jax
import jax.numpy as jnp
from jax import lax
from jax.experimental import pallas as pl
from jax.experimental.pallas import tpu as pltpu
from jax.sharding import PartitionSpec as P

MESH = pl.DeviceIdType.MESH
F32 = jnp.float32
BF16 = jnp.bfloat16

NX = 4
NZ = 8
NBAND = 8
PROJ = 512
ATOMS = 64
NSPEC = 4
KMAX = 18
GL = 1024
BL = 256
CH = 128
NCH = BL // CH
QR = PROJ // NX
SR = QR // NZ

FAR_FIRST = (4, 3, 5, 2, 6, 1, 7)
NEAR_FIRST = (1, 7, 2, 6, 3, 5, 4)

KINETIC_SCALE = 0.005
EPSILON = 1e-6

SIN_C = (3.141592653589793, -5.16771278004997, 2.550164039877345, -0.5992645293207921, 0.08214588661112823, -0.00737043094571435, 0.00046630280576761255)
COS_C = (1.0, -4.934802200544679, 4.058712126416768, -1.3352627688545893, 0.2353306303588935, -0.02580689139001406, 0.0019295743094039231)


def split(x):
    hi = x.astype(BF16)
    return hi, (x - hi.astype(F32)).astype(BF16)


def dot(a, b):
    return jnp.dot(a, b, preferred_element_type=F32)


def dot3(ah, al, bh, bl):
    return dot(ah, bh) + dot(al, bh) + dot(ah, bl)


def horner(coeffs, x):
    acc = jnp.full_like(x, coeffs[-1])
    for c in coeffs[-2::-1]:
        acc = acc * x + c
    return acc


def iota(shape, dim):
    return lax.broadcasted_iota(jnp.int32, shape, dim)


def kernel(waves, miller_in, pos_in, ff_in, coup_in, spec_in, size_in, occ_in,
           res, est_to, en_out,
           psi, bh, bl, th, tl, vh, vl, dh, dl, mh, ml,
           ffs, ffk, ctk, stk, cks, ckk, kcol, pbuf, xr, q, zr, full, rbuf,
           knx, knz, kna, ebuf, miller, pos, ff, coup, spec, size, occ, est_out,
           in_sem, est_sem, out_sem, sent, xr_sem, zr_sem, za_sem, xa_sem, kn_sem):
    gi = lax.axis_index("ga")
    band = lax.axis_index("band")
    z = lax.div(gi, NX)
    x = lax.rem(gi, NX)
    r, o, l = (lax.rem(x + k, NX) for k in (1, 2, 3))

    def at_x(xx):
        return {"ga": z * NX + xx}

    def at_z(k):
        return {"ga": lax.rem(z + k, NZ) * NX + x}

    def at_band(k):
        return {"band": lax.rem(band + k, NBAND)}

    smalls = [
        pltpu.make_async_copy(a, b, in_sem.at[2 + i])
        for i, (a, b) in enumerate((
            (size_in, size), (spec_in, spec), (pos_in, pos), (miller_in, miller),
            (ff_in, ff), (coup_in, coup), (occ_in, occ),
        ))
    ]
    loads = [pltpu.make_async_copy(waves.at[i], psi.at[i], in_sem.at[i]) for i in range(2)]
    for c in smalls + loads:
        c.start()

    barrier = pltpu.get_barrier_semaphore()
    peers = [at_x(r), at_x(l), at_x(o)] + [at_z(k) for k in range(1, NZ)] + [at_band(k) for k in range(1, NBAND)]
    for p in peers:
        pl.semaphore_signal(barrier, inc=1, device_id=p, device_id_type=MESH)

    def remote(src, dst, where, recv_sem, send_sem=None):
        copy = pltpu.make_async_remote_copy(
            src_ref=src, dst_ref=dst, send_sem=sent.at[0] if send_sem is None else send_sem,
            recv_sem=recv_sem, device_id=where, device_id_type=MESH,
        )
        copy.start()
        return copy

    def arrived(ref, sem):
        pltpu.make_async_copy(ref, ref, sem).wait()

    for c in smalls:
        c.wait()
    size_row = size[...].astype(F32)
    spec_row = spec[...].astype(F32)
    i0, i1 = iota((ATOMS, ATOMS), 0), iota((ATOMS, ATOMS), 1)
    size_col = jnp.sum(jnp.where(i0 == i1, size_row, 0.0), axis=1, keepdims=True)
    end_row = jnp.sum(jnp.where(i0 <= i1, size_col, 0.0), axis=0, keepdims=True)
    end_col = jnp.sum(jnp.where(i1 <= i0, size_row, 0.0), axis=1, keepdims=True)
    start_row = end_row - size_row
    start_col = end_col - size_col
    p_col = iota((PROJ, ATOMS), 0).astype(F32)
    own = (p_col >= start_row) & (p_col < end_row)
    atom_row = iota((1, ATOMS), 1).astype(F32)
    owner_col = jnp.sum(jnp.where(own, atom_row, 0.0), axis=1, keepdims=True)
    row_col = jnp.sum(jnp.where(own, spec_row + NSPEC * (p_col - start_row), 0.0), axis=1, keepdims=True)
    lane = iota((PROJ, 256), 1)
    row_hot = jnp.where((lane & 127).astype(F32) == row_col, 1.0, 0.0).astype(BF16)
    own_hot = jnp.where((lane[:, :128] & 63).astype(F32) == owner_col, 1.0, 0.0).astype(BF16)

    ffs[72:80, :] = jnp.zeros((8, GL), F32)
    for k in range(KMAX):
        ffs[k * NSPEC:(k + 1) * NSPEC, :] = ff[k]
    for g in range(0, 256, 128):
        ffk[g + 80:g + 128, :] = jnp.zeros((48, GL), BF16)
    ffk[0:80, :], ffk[128:208, :] = split(ffs[...])
    pos_col = [
        jnp.sum(jnp.where(i0 == i1, pos[i:i + 1, :], 0.0), axis=1, keepdims=True) for i in range(3)
    ]
    m = miller[...].astype(F32)
    for g in range(0, GL, 256):
        mg = m[:, g:g + 256]
        turns = pos_col[0] * mg[0:1] + pos_col[1] * mg[1:2] + pos_col[2] * mg[2:3]
        turns = turns - jnp.round(turns)
        t2 = turns * turns
        sh = horner(SIN_C, t2) * turns
        ch = horner(COS_C, t2)
        for dst, val in ((ctk, 1.0 - 2.0 * (sh * sh)), (stk, 2.0 * (sh * ch))):
            a, b = split(val)
            dst[0:64, g:g + 256] = a
            dst[64:128, g:g + 256] = b
        radial = dot(row_hot, ffk[:, g:g + 256])
        for base, tab, sign in ((0, ctk, 1.0), (GL, stk, -1.0)):
            b = radial * dot(own_hot, tab[:, g:g + 256])
            b = b if sign > 0 else -b
            a, b = split(b)
            bh[:, base + g:base + g + 256] = a
            bl[:, base + g:base + g + 256] = b
    ksum = m[0:1] * m[0:1] + m[1:2] * m[1:2] + m[2:3] * m[2:3]
    krow = jnp.broadcast_to(0.5 * KINETIC_SCALE * ksum, (128, GL))
    for g in range(0, GL, 128):
        kcol[g:g + 128, :] = jnp.transpose(krow[:, g:g + 128])

    for c in loads:
        c.wait()

    def project(c):
        cols = slice(c * CH, (c + 1) * CH)
        rows = 256
        kin = jnp.zeros((1, CH), F32)
        nrm = jnp.zeros((1, CH), F32)
        for g in range(0, GL, rows):
            pr = psi[0, g:g + rows, cols]
            pi = psi[1, g:g + rows, cols]
            den = pr * pr + pi * pi
            nrm = nrm + jnp.sum(den, axis=0, keepdims=True)
            kin = kin + jnp.sum(kcol[g:g + rows, :] * den, axis=0, keepdims=True)
            for buf, (a, b) in zip((vh, vl), zip(split(pr), split(pi))):
                buf[g:g + rows, 0:CH] = a
                buf[g:g + rows, CH:2 * CH] = b
                buf[GL + g:GL + g + rows, 0:CH] = b
                buf[GL + g:GL + g + rows, CH:2 * CH] = -a
        p = dot3(bh[...], bl[...], vh[...], vl[...])
        pbuf[c, 0] = p[:, :CH]
        pbuf[c, 1] = p[:, CH:]
        return kin, nrm

    def rows_of(xx, zz):
        return pl.ds(pl.multiple_of(xx * QR + zz * SR, SR), SR)

    def z_at(k):
        return lax.rem(z + k, NZ)

    def x_at(k):
        return lax.rem(x + k, NX)

    def x_first(c):
        for k in FAR_FIRST + (0,):
            for d in (2, 1, 3):
                part = pbuf.at[c, :, rows_of(x_at(d), z_at(k)), :]
                remote(part, xr.at[c, k, d - 1], at_x(x_at(d)), xr_sem.at[c, k])

    def z_first(c):
        for k in FAR_FIRST + (0,):
            arrived(xr.at[c, k], xr_sem.at[c, k])
            q[c, k] = pbuf[c, :, rows_of(x, z_at(k)), :] + xr[c, k, 0] + xr[c, k, 1] + xr[c, k, 2]
            if k:
                remote(q.at[c, k], zr.at[c, k - 1], at_z(k), zr_sem.at[c])

    mine = rows_of(x, z)

    def spread(c, zz):
        part = full.at[c, :, rows_of(x, zz), :]
        for d in (2, 1, 3):
            remote(part, part, at_x(x_at(d)), xa_sem.at[c])

    def z_back(c):
        arrived(zr.at[c], zr_sem.at[c])
        share = q[c, 0]
        for k in range(NZ - 1):
            share = share + zr[c, k]
        full[c, :, mine, :] = share
        part = full.at[c, :, mine, :]
        spread(c, z)
        return {k: remote(part, part, at_z(k), za_sem.at[c, k - 1]) for k in NEAR_FIRST}

    def x_back(c, back):
        for k in NEAR_FIRST:
            back[k].wait_recv()
            spread(c, z_at(NZ - k))

    kn0 = project(0)
    pl.semaphore_wait(barrier, len(peers))
    x_first(0)
    kn1 = project(1)
    x_first(1)

    tile_row = iota((8, CH), 0)
    kn = jnp.zeros((8, CH), F32)
    for i, v in enumerate((kn0[0], kn0[1], kn1[0], kn1[1])):
        kn = jnp.where(tile_row == i, v, kn)
    knx[x] = kn
    for k in (r, l, o):
        remote(knx.at[x], knx.at[x], at_x(k), kn_sem.at[0], sent.at[1])

    cks[...] = jnp.zeros_like(cks)
    for k in range(KMAX):
        cks[k * NSPEC:(k + 1) * NSPEC, 0:KMAX] = coup[k]
    ckk[0:128, :], ckk[128:256, :] = split(cks[...])
    q_row = iota((ATOMS, PROJ), 1).astype(F32)
    own_t = (q_row >= start_col) & (q_row < end_col)
    atom_col = iota((ATOMS, 1), 0).astype(F32)
    owner_row = jnp.sum(jnp.where(own_t, atom_col, 0.0), axis=0, keepdims=True)
    chan_row = jnp.sum(jnp.where(own_t, q_row - start_col, 0.0), axis=0, keepdims=True)
    chan_hot = jnp.where(iota((128, PROJ), 0).astype(F32) == chan_row, 1.0, 0.0).astype(BF16)
    same = owner_col == owner_row
    for dst, part in ((dh, row_hot[:, :128]), (dl, row_hot[:, 128:])):
        base = 0 if dst is dh else 128
        table = dot(part, ckk[base:base + 128, :]).astype(BF16)
        dst[...] = jnp.where(same, dot(table, chan_hot), 0.0).astype(BF16)

    def turned(g):
        for src, dst in ((bh, th), (bl, tl)):
            for half in range(2):
                dst[g:g + 256, half * PROJ:(half + 1) * PROJ] = jnp.transpose(
                    src[:, half * GL + g:half * GL + g + 256]
                )

    for g in range(0, GL, 256):
        turned(g)

    z_first(0)

    z_first(1)
    arrived(knx.at[0:NX - 1], kn_sem.at[0])
    knz[z] = knx[0] + knx[1] + knx[2] + knx[3]
    for k in range(1, NZ):
        remote(knz.at[z], knz.at[z], at_z(k), kn_sem.at[1], sent.at[1])


    back0 = z_back(0)
    x_back(0, back0)
    back1 = z_back(1)
    x_back(1, back1)
    arrived(knz.at[0:NZ - 1], kn_sem.at[1])
    tot = knz[0]
    for k in range(1, NZ):
        tot = tot + knz[k]
    kna[...] = tot

    def finish(c):
        arrived(full.at[c, :, 0:PROJ - QR, :], xa_sem.at[c])
        cols = slice(c * CH, (c + 1) * CH)
        for i in range(2):
            a, b = split(full[c, i])
            mh[0:PROJ, i * CH:(i + 1) * CH] = a
            ml[0:PROJ, i * CH:(i + 1) * CH] = b
        mix = dot3(dh[...], dl[...], mh[0:PROJ, :], ml[0:PROJ, :])
        mr, mi = mix[:, :CH], mix[:, CH:]
        nonlocal_ = jnp.sum(full[c, 0] * mr + full[c, 1] * mi, axis=0, keepdims=True)
        for buf, (a, b) in zip((mh, ml), zip(split(mr), split(mi))):
            buf[0:PROJ, 0:CH] = a
            buf[0:PROJ, CH:2 * CH] = b
            buf[PROJ:2 * PROJ, 0:CH] = -b
            buf[PROJ:2 * PROJ, CH:2 * CH] = a
        kin, nrm = kna[2 * c:2 * c + 1, :], kna[2 * c + 1:2 * c + 2, :]
        est = (kin + nonlocal_) / (nrm + EPSILON)
        est_out[:, cols] = est
        energy = occ[:, cols] * nonlocal_ / (nrm + EPSILON)
        return est, energy

    def residual(c, est):
        cols = slice(c * CH, (c + 1) * CH)
        out = []
        acc = dot3(th[...], tl[...], mh[...], ml[...])
        for i in range(2):
            rbuf[i, :, cols] = (kcol[...] - est) * psi[i, :, cols] + acc[:, i * CH:(i + 1) * CH]
            copy = pltpu.make_async_copy(rbuf.at[i, :, cols], res.at[i, :, cols], out_sem.at[c, i])
            copy.start()
            out.append(copy)
        return out

    est0, en0 = finish(0)
    outs = residual(0, est0)
    est1, en1 = finish(1)
    ebuf[band] = jnp.broadcast_to(en0 + en1, (8, CH))
    for k in range(1, NBAND):
        remote(ebuf.at[band], ebuf.at[band], at_band(k), kn_sem.at[2], sent.at[1])
    est_copy = pltpu.make_async_copy(est_out, est_to, est_sem)
    est_copy.start()
    outs += residual(1, est1) + [est_copy]
    arrived(ebuf.at[0:NBAND - 1], kn_sem.at[2])
    total = ebuf[0]
    for k in range(1, NBAND):
        total = total + ebuf[k]
    en_out[0, 0] = jnp.sum(total[0:1, :])
    arrived(rbuf.at[:, 0:NPIECE * 8, :], sent.at[0])
    arrived(pbuf.at[0, 0, 0:NTILE * 8, :], sent.at[1])
    for w in outs:
        w.wait()


NPIECE = NCH * (24 + 7 + 7 + 24)
NTILE = 3 + 7 + 7


def on_device(waves, miller, positions, form_factors, coupling, species, block_sizes, occupation):
    anywhere = pl.BlockSpec(memory_space=pl.ANY)
    res, est, en = pl.pallas_call(
        kernel,
        out_shape=(
            jax.ShapeDtypeStruct((2, GL, BL), F32),
            jax.ShapeDtypeStruct((1, BL), F32),
            jax.ShapeDtypeStruct((1, 1), F32),
        ),
        in_specs=[anywhere] * 8,
        out_specs=(
            anywhere,
            anywhere,
            pl.BlockSpec(memory_space=pltpu.SMEM),
        ),
        scratch_shapes=[
            pltpu.VMEM((2, GL, BL), F32),
            pltpu.VMEM((PROJ, 2 * GL), BF16),
            pltpu.VMEM((PROJ, 2 * GL), BF16),
            pltpu.VMEM((GL, 2 * PROJ), BF16),
            pltpu.VMEM((GL, 2 * PROJ), BF16),
            pltpu.VMEM((2 * GL, 2 * CH), BF16),
            pltpu.VMEM((2 * GL, 2 * CH), BF16),
            pltpu.VMEM((PROJ, PROJ), BF16),
            pltpu.VMEM((PROJ, PROJ), BF16),
            pltpu.VMEM((2 * PROJ, 2 * CH), BF16),
            pltpu.VMEM((2 * PROJ, 2 * CH), BF16),
            pltpu.VMEM((80, GL), F32),
            pltpu.VMEM((256, GL), BF16),
            pltpu.VMEM((128, GL), BF16),
            pltpu.VMEM((128, GL), BF16),
            pltpu.VMEM((128, 128), F32),
            pltpu.VMEM((256, 128), BF16),
            pltpu.VMEM((GL, CH), F32),
            pltpu.VMEM((NCH, 2, PROJ, CH), F32),
            pltpu.VMEM((NCH, NZ, NX - 1, 2, SR, CH), F32),
            pltpu.VMEM((NCH, NZ, 2, SR, CH), F32),
            pltpu.VMEM((NCH, NZ - 1, 2, SR, CH), F32),
            pltpu.VMEM((NCH, 2, PROJ, CH), F32),
            pltpu.VMEM((2, GL, BL), F32),
            pltpu.VMEM((NX, 8, CH), F32),
            pltpu.VMEM((NZ, 8, CH), F32),
            pltpu.VMEM((8, CH), F32),
            pltpu.VMEM((NBAND, 8, CH), F32),
            pltpu.VMEM((3, GL), jnp.int32),
            pltpu.VMEM((3, ATOMS), F32),
            pltpu.VMEM((KMAX, NSPEC, GL), F32),
            pltpu.VMEM((KMAX, NSPEC, KMAX), F32),
            pltpu.VMEM((1, ATOMS), jnp.int32),
            pltpu.VMEM((1, ATOMS), jnp.int32),
            pltpu.VMEM((1, BL), F32),
            pltpu.VMEM((1, BL), F32),
            pltpu.SemaphoreType.DMA((9,)),
            pltpu.SemaphoreType.DMA,
            pltpu.SemaphoreType.DMA((NCH, 2)),
            pltpu.SemaphoreType.DMA((2,)),
            pltpu.SemaphoreType.DMA((NCH, NZ)),
            pltpu.SemaphoreType.DMA((NCH,)),
            pltpu.SemaphoreType.DMA((NCH, NZ - 1)),
            pltpu.SemaphoreType.DMA((NCH,)),
            pltpu.SemaphoreType.DMA((3,)),
        ],
        compiler_params=pltpu.CompilerParams(
            collective_id=0, has_side_effects=True, vmem_limit_bytes=60000 * 1024
        ),
    )(
        waves, miller, positions.T, form_factors.transpose(1, 0, 2), coupling.transpose(1, 0, 2),
        species.reshape(1, -1), block_sizes.reshape(1, -1), occupation.reshape(1, -1),
    )
    return res, est.reshape(BL), en.reshape(())


def solution(mesh):
    in_specs = (
        P(None, "ga", "band"),
        P(None, "ga"),
        P(),
        P(None, None, "ga"),
        P(),
        P(),
        P(),
        P("band"),
    )
    out_specs = (P(None, "ga", "band"), P("band"), P())
    return jax.shard_map(
        on_device, mesh=mesh, in_specs=in_specs, out_specs=out_specs, check_vma=False
    )
```

```python
import jax
import jax.numpy as jnp
from jax import lax
from jax.experimental import pallas as pl
from jax.experimental.pallas import tpu as pltpu
from jax.sharding import PartitionSpec as P

MESH = pl.DeviceIdType.MESH
F32 = jnp.float32
BF16 = jnp.bfloat16

NX = 4
NZ = 8
NBAND = 8
PROJ = 512
ATOMS = 64
NSPEC = 4
KMAX = 18
GL = 1024
BL = 256
CH = 128
NCH = BL // CH
QR = PROJ // NX
SR = QR // NZ

FAR_FIRST = (4, 3, 5, 2, 6, 1, 7)
NEAR_FIRST = (1, 7, 2, 6, 3, 5, 4)

KINETIC_SCALE = 0.005
EPSILON = 1e-6

SIN_C = (3.141592653589793, -5.16771278004997, 2.550164039877345, -0.5992645293207921, 0.08214588661112823, -0.00737043094571435, 0.00046630280576761255)
COS_C = (1.0, -4.934802200544679, 4.058712126416768, -1.3352627688545893, 0.2353306303588935, -0.02580689139001406, 0.0019295743094039231)


def split(x):
    hi = x.astype(BF16)
    return hi, (x - hi.astype(F32)).astype(BF16)


def dot(a, b):
    return jnp.dot(a, b, preferred_element_type=F32)


def dot3(ah, al, bh, bl):
    return dot(ah, bh) + dot(al, bh) + dot(ah, bl)


def horner(coeffs, x):
    acc = jnp.full_like(x, coeffs[-1])
    for c in coeffs[-2::-1]:
        acc = acc * x + c
    return acc


def iota(shape, dim):
    return lax.broadcasted_iota(jnp.int32, shape, dim)


def kernel(waves, miller_in, pos_in, ff_in, coup_in, spec_in, size_in, occ_in,
           res, est_to, en_out,
           psi, bh, bl, th, tl, vh, vl, dh, dl, mh, ml,
           ffs, ffk, ctk, stk, cks, ckk, kcol, pbuf, xr, q, zr, full, rbuf,
           knx, knz, kna, ebuf, miller, pos, ff, coup, spec, size, occ, est_out,
           in_sem, est_sem, out_sem, sent, xr_sem, zr_sem, za_sem, xa_sem, kn_sem):
    gi = lax.axis_index("ga")
    band = lax.axis_index("band")
    z = lax.div(gi, NX)
    x = lax.rem(gi, NX)
    r, o, l = (lax.rem(x + k, NX) for k in (1, 2, 3))

    def at_x(xx):
        return {"ga": z * NX + xx}

    def at_z(k):
        return {"ga": lax.rem(z + k, NZ) * NX + x}

    def at_band(k):
        return {"band": lax.rem(band + k, NBAND)}

    smalls = [
        pltpu.make_async_copy(a, b, in_sem.at[2 + i])
        for i, (a, b) in enumerate((
            (size_in, size), (spec_in, spec), (pos_in, pos), (miller_in, miller),
            (ff_in, ff), (coup_in, coup), (occ_in, occ),
        ))
    ]
    loads = [pltpu.make_async_copy(waves.at[i], psi.at[i], in_sem.at[i]) for i in range(2)]
    for c in smalls + loads:
        c.start()

    barrier = pltpu.get_barrier_semaphore()
    peers = [at_x(r), at_x(l), at_x(o)] + [at_z(k) for k in range(1, NZ)] + [at_band(k) for k in range(1, NBAND)]
    for p in peers:
        pl.semaphore_signal(barrier, inc=1, device_id=p, device_id_type=MESH)

    def remote(src, dst, where, recv_sem, send_sem=None):
        copy = pltpu.make_async_remote_copy(
            src_ref=src, dst_ref=dst, send_sem=sent.at[0] if send_sem is None else send_sem,
            recv_sem=recv_sem, device_id=where, device_id_type=MESH,
        )
        copy.start()
        return copy

    def arrived(ref, sem):
        pltpu.make_async_copy(ref, ref, sem).wait()

    for c in smalls:
        c.wait()
    size_row = size[...].astype(F32)
    spec_row = spec[...].astype(F32)
    i0, i1 = iota((ATOMS, ATOMS), 0), iota((ATOMS, ATOMS), 1)
    size_col = jnp.sum(jnp.where(i0 == i1, size_row, 0.0), axis=1, keepdims=True)
    end_row = jnp.sum(jnp.where(i0 <= i1, size_col, 0.0), axis=0, keepdims=True)
    end_col = jnp.sum(jnp.where(i1 <= i0, size_row, 0.0), axis=1, keepdims=True)
    start_row = end_row - size_row
    start_col = end_col - size_col
    p_col = iota((PROJ, ATOMS), 0).astype(F32)
    own = (p_col >= start_row) & (p_col < end_row)
    atom_row = iota((1, ATOMS), 1).astype(F32)
    owner_col = jnp.sum(jnp.where(own, atom_row, 0.0), axis=1, keepdims=True)
    row_col = jnp.sum(jnp.where(own, spec_row + NSPEC * (p_col - start_row), 0.0), axis=1, keepdims=True)
    lane = iota((PROJ, 256), 1)
    row_hot = jnp.where((lane & 127).astype(F32) == row_col, 1.0, 0.0).astype(BF16)
    own_hot = jnp.where((lane[:, :128] & 63).astype(F32) == owner_col, 1.0, 0.0).astype(BF16)

    ffs[72:80, :] = jnp.zeros((8, GL), F32)
    for k in range(KMAX):
        ffs[k * NSPEC:(k + 1) * NSPEC, :] = ff[k]
    for g in range(0, 256, 128):
        ffk[g + 80:g + 128, :] = jnp.zeros((48, GL), BF16)
    ffk[0:80, :], ffk[128:208, :] = split(ffs[...])
    pos_col = [
        jnp.sum(jnp.where(i0 == i1, pos[i:i + 1, :], 0.0), axis=1, keepdims=True) for i in range(3)
    ]
    m = miller[...].astype(F32)
    for g in range(0, GL, 256):
        mg = m[:, g:g + 256]
        turns = pos_col[0] * mg[0:1] + pos_col[1] * mg[1:2] + pos_col[2] * mg[2:3]
        turns = turns - jnp.round(turns)
        t2 = turns * turns
        sh = horner(SIN_C, t2) * turns
        ch = horner(COS_C, t2)
        for dst, val in ((ctk, 1.0 - 2.0 * (sh * sh)), (stk, 2.0 * (sh * ch))):
            a, b = split(val)
            dst[0:64, g:g + 256] = a
            dst[64:128, g:g + 256] = b
        radial = dot(row_hot, ffk[:, g:g + 256])
        for base, tab, sign in ((0, ctk, 1.0), (GL, stk, -1.0)):
            b = radial * dot(own_hot, tab[:, g:g + 256])
            b = b if sign > 0 else -b
            a, b = split(b)
            bh[:, base + g:base + g + 256] = a
            bl[:, base + g:base + g + 256] = b
    ksum = m[0:1] * m[0:1] + m[1:2] * m[1:2] + m[2:3] * m[2:3]
    krow = jnp.broadcast_to(0.5 * KINETIC_SCALE * ksum, (128, GL))
    for g in range(0, GL, 128):
        kcol[g:g + 128, :] = jnp.transpose(krow[:, g:g + 128])

    for c in loads:
        c.wait()

    def project(c):
        cols = slice(c * CH, (c + 1) * CH)
        rows = 256
        kin = jnp.zeros((1, CH), F32)
        nrm = jnp.zeros((1, CH), F32)
        for g in range(0, GL, rows):
            pr = psi[0, g:g + rows, cols]
            pi = psi[1, g:g + rows, cols]
            den = pr * pr + pi * pi
            nrm = nrm + jnp.sum(den, axis=0, keepdims=True)
            kin = kin + jnp.sum(kcol[g:g + rows, :] * den, axis=0, keepdims=True)
            for buf, (a, b) in zip((vh, vl), zip(split(pr), split(pi))):
                buf[g:g + rows, 0:CH] = a
                buf[g:g + rows, CH:2 * CH] = b
                buf[GL + g:GL + g + rows, 0:CH] = b
                buf[GL + g:GL + g + rows, CH:2 * CH] = -a
        return kin, nrm

    def projected(c, rows):
        p = dot3(bh[rows, :], bl[rows, :], vh[...], vl[...])
        pbuf[c, 0, rows, :] = p[:, :CH]
        pbuf[c, 1, rows, :] = p[:, CH:]

    def rows_of(xx, zz):
        return pl.ds(pl.multiple_of(xx * QR + zz * SR, SR), SR)

    def z_at(k):
        return lax.rem(z + k, NZ)

    def x_at(k):
        return lax.rem(x + k, NX)

    def x_first(c, to=(2, 1, 3)):
        for k in FAR_FIRST + (0,):
            for d in to:
                part = pbuf.at[c, :, rows_of(x_at(d), z_at(k)), :]
                remote(part, xr.at[c, k, d - 1], at_x(x_at(d)), xr_sem.at[c, k])

    def z_first(c):
        for k in FAR_FIRST + (0,):
            arrived(xr.at[c, k], xr_sem.at[c, k])
            q[c, k] = pbuf[c, :, rows_of(x, z_at(k)), :] + xr[c, k, 0] + xr[c, k, 1] + xr[c, k, 2]
            if k:
                remote(q.at[c, k], zr.at[c, k - 1], at_z(k), zr_sem.at[c])

    mine = rows_of(x, z)

    def spread(c, zz):
        part = full.at[c, :, rows_of(x, zz), :]
        for d in (2, 1, 3):
            remote(part, part, at_x(x_at(d)), xa_sem.at[c])

    def z_back(c):
        arrived(zr.at[c], zr_sem.at[c])
        share = q[c, 0]
        for k in range(NZ - 1):
            share = share + zr[c, k]
        full[c, :, mine, :] = share
        part = full.at[c, :, mine, :]
        spread(c, z)
        return {k: remote(part, part, at_z(k), za_sem.at[c, k - 1]) for k in NEAR_FIRST}

    def x_back(c, back):
        for k in NEAR_FIRST:
            back[k].wait_recv()
            spread(c, z_at(NZ - k))

    kn0 = project(0)
    for i, d in enumerate((2, 1, 3, 0)):
        projected(0, pl.ds(pl.multiple_of(x_at(d) * QR, QR), QR))
        if i == 0:
            pl.semaphore_wait(barrier, len(peers))
        if d:
            x_first(0, (d,))
    kn1 = project(1)
    projected(1, slice(0, PROJ))
    x_first(1)

    tile_row = iota((8, CH), 0)
    kn = jnp.zeros((8, CH), F32)
    for i, v in enumerate((kn0[0], kn0[1], kn1[0], kn1[1])):
        kn = jnp.where(tile_row == i, v, kn)
    knx[x] = kn
    for k in (r, l, o):
        remote(knx.at[x], knx.at[x], at_x(k), kn_sem.at[0], sent.at[1])

    cks[...] = jnp.zeros_like(cks)
    for k in range(KMAX):
        cks[k * NSPEC:(k + 1) * NSPEC, 0:KMAX] = coup[k]
    ckk[0:128, :], ckk[128:256, :] = split(cks[...])
    q_row = iota((ATOMS, PROJ), 1).astype(F32)
    own_t = (q_row >= start_col) & (q_row < end_col)
    atom_col = iota((ATOMS, 1), 0).astype(F32)
    owner_row = jnp.sum(jnp.where(own_t, atom_col, 0.0), axis=0, keepdims=True)
    chan_row = jnp.sum(jnp.where(own_t, q_row - start_col, 0.0), axis=0, keepdims=True)
    chan_hot = jnp.where(iota((128, PROJ), 0).astype(F32) == chan_row, 1.0, 0.0).astype(BF16)
    same = owner_col == owner_row
    for dst, part in ((dh, row_hot[:, :128]), (dl, row_hot[:, 128:])):
        base = 0 if dst is dh else 128
        table = dot(part, ckk[base:base + 128, :]).astype(BF16)
        dst[...] = jnp.where(same, dot(table, chan_hot), 0.0).astype(BF16)

    def turned(g):
        for src, dst in ((bh, th), (bl, tl)):
            for half in range(2):
                dst[g:g + 256, half * PROJ:(half + 1) * PROJ] = jnp.transpose(
                    src[:, half * GL + g:half * GL + g + 256]
                )

    for g in range(0, GL, 256):
        turned(g)

    z_first(0)

    z_first(1)
    arrived(knx.at[0:NX - 1], kn_sem.at[0])
    knz[z] = knx[0] + knx[1] + knx[2] + knx[3]
    for k in range(1, NZ):
        remote(knz.at[z], knz.at[z], at_z(k), kn_sem.at[1], sent.at[1])


    back0 = z_back(0)
    x_back(0, back0)
    back1 = z_back(1)
    x_back(1, back1)
    arrived(knz.at[0:NZ - 1], kn_sem.at[1])
    tot = knz[0]
    for k in range(1, NZ):
        tot = tot + knz[k]
    kna[...] = tot

    def finish(c):
        arrived(full.at[c, :, 0:PROJ - QR, :], xa_sem.at[c])
        cols = slice(c * CH, (c + 1) * CH)
        for i in range(2):
            a, b = split(full[c, i])
            mh[0:PROJ, i * CH:(i + 1) * CH] = a
            ml[0:PROJ, i * CH:(i + 1) * CH] = b
        mix = dot3(dh[...], dl[...], mh[0:PROJ, :], ml[0:PROJ, :])
        mr, mi = mix[:, :CH], mix[:, CH:]
        nonlocal_ = jnp.sum(full[c, 0] * mr + full[c, 1] * mi, axis=0, keepdims=True)
        for buf, (a, b) in zip((mh, ml), zip(split(mr), split(mi))):
            buf[0:PROJ, 0:CH] = a
            buf[0:PROJ, CH:2 * CH] = b
            buf[PROJ:2 * PROJ, 0:CH] = -b
            buf[PROJ:2 * PROJ, CH:2 * CH] = a
        kin, nrm = kna[2 * c:2 * c + 1, :], kna[2 * c + 1:2 * c + 2, :]
        est = (kin + nonlocal_) / (nrm + EPSILON)
        est_out[:, cols] = est
        energy = occ[:, cols] * nonlocal_ / (nrm + EPSILON)
        return est, energy

    def residual(c, est):
        cols = slice(c * CH, (c + 1) * CH)
        out = []
        acc = dot3(th[...], tl[...], mh[...], ml[...])
        for i in range(2):
            rbuf[i, :, cols] = (kcol[...] - est) * psi[i, :, cols] + acc[:, i * CH:(i + 1) * CH]
            copy = pltpu.make_async_copy(rbuf.at[i, :, cols], res.at[i, :, cols], out_sem.at[c, i])
            copy.start()
            out.append(copy)
        return out

    est0, en0 = finish(0)
    outs = residual(0, est0)
    est1, en1 = finish(1)
    ebuf[band] = jnp.broadcast_to(en0 + en1, (8, CH))
    for k in range(1, NBAND):
        remote(ebuf.at[band], ebuf.at[band], at_band(k), kn_sem.at[2], sent.at[1])
    est_copy = pltpu.make_async_copy(est_out, est_to, est_sem)
    est_copy.start()
    outs += residual(1, est1) + [est_copy]
    arrived(ebuf.at[0:NBAND - 1], kn_sem.at[2])
    total = ebuf[0]
    for k in range(1, NBAND):
        total = total + ebuf[k]
    en_out[0, 0] = jnp.sum(total[0:1, :])
    arrived(rbuf.at[:, 0:NPIECE * 8, :], sent.at[0])
    arrived(pbuf.at[0, 0, 0:NTILE * 8, :], sent.at[1])
    for w in outs:
        w.wait()


NPIECE = NCH * (24 + 7 + 7 + 24)
NTILE = 3 + 7 + 7


def on_device(waves, miller, positions, form_factors, coupling, species, block_sizes, occupation):
    anywhere = pl.BlockSpec(memory_space=pl.ANY)
    res, est, en = pl.pallas_call(
        kernel,
        out_shape=(
            jax.ShapeDtypeStruct((2, GL, BL), F32),
            jax.ShapeDtypeStruct((1, BL), F32),
            jax.ShapeDtypeStruct((1, 1), F32),
        ),
        in_specs=[anywhere] * 8,
        out_specs=(
            anywhere,
            anywhere,
            pl.BlockSpec(memory_space=pltpu.SMEM),
        ),
        scratch_shapes=[
            pltpu.VMEM((2, GL, BL), F32),
            pltpu.VMEM((PROJ, 2 * GL), BF16),
            pltpu.VMEM((PROJ, 2 * GL), BF16),
            pltpu.VMEM((GL, 2 * PROJ), BF16),
            pltpu.VMEM((GL, 2 * PROJ), BF16),
            pltpu.VMEM((2 * GL, 2 * CH), BF16),
            pltpu.VMEM((2 * GL, 2 * CH), BF16),
            pltpu.VMEM((PROJ, PROJ), BF16),
            pltpu.VMEM((PROJ, PROJ), BF16),
            pltpu.VMEM((2 * PROJ, 2 * CH), BF16),
            pltpu.VMEM((2 * PROJ, 2 * CH), BF16),
            pltpu.VMEM((80, GL), F32),
            pltpu.VMEM((256, GL), BF16),
            pltpu.VMEM((128, GL), BF16),
            pltpu.VMEM((128, GL), BF16),
            pltpu.VMEM((128, 128), F32),
            pltpu.VMEM((256, 128), BF16),
            pltpu.VMEM((GL, CH), F32),
            pltpu.VMEM((NCH, 2, PROJ, CH), F32),
            pltpu.VMEM((NCH, NZ, NX - 1, 2, SR, CH), F32),
            pltpu.VMEM((NCH, NZ, 2, SR, CH), F32),
            pltpu.VMEM((NCH, NZ - 1, 2, SR, CH), F32),
            pltpu.VMEM((NCH, 2, PROJ, CH), F32),
            pltpu.VMEM((2, GL, BL), F32),
            pltpu.VMEM((NX, 8, CH), F32),
            pltpu.VMEM((NZ, 8, CH), F32),
            pltpu.VMEM((8, CH), F32),
            pltpu.VMEM((NBAND, 8, CH), F32),
            pltpu.VMEM((3, GL), jnp.int32),
            pltpu.VMEM((3, ATOMS), F32),
            pltpu.VMEM((KMAX, NSPEC, GL), F32),
            pltpu.VMEM((KMAX, NSPEC, KMAX), F32),
            pltpu.VMEM((1, ATOMS), jnp.int32),
            pltpu.VMEM((1, ATOMS), jnp.int32),
            pltpu.VMEM((1, BL), F32),
            pltpu.VMEM((1, BL), F32),
            pltpu.SemaphoreType.DMA((9,)),
            pltpu.SemaphoreType.DMA,
            pltpu.SemaphoreType.DMA((NCH, 2)),
            pltpu.SemaphoreType.DMA((2,)),
            pltpu.SemaphoreType.DMA((NCH, NZ)),
            pltpu.SemaphoreType.DMA((NCH,)),
            pltpu.SemaphoreType.DMA((NCH, NZ - 1)),
            pltpu.SemaphoreType.DMA((NCH,)),
            pltpu.SemaphoreType.DMA((3,)),
        ],
        compiler_params=pltpu.CompilerParams(
            collective_id=0, has_side_effects=True, vmem_limit_bytes=60000 * 1024
        ),
    )(
        waves, miller, positions.T, form_factors.transpose(1, 0, 2), coupling.transpose(1, 0, 2),
        species.reshape(1, -1), block_sizes.reshape(1, -1), occupation.reshape(1, -1),
    )
    return res, est.reshape(BL), en.reshape(())


def solution(mesh):
    in_specs = (
        P(None, "ga", "band"),
        P(None, "ga"),
        P(),
        P(None, None, "ga"),
        P(),
        P(),
        P(),
        P("band"),
    )
    out_specs = (P(None, "ga", "band"), P("band"), P())
    return jax.shard_map(
        on_device, mesh=mesh, in_specs=in_specs, out_specs=out_specs, check_vma=False
    )
```

```python
import jax
import jax.numpy as jnp
from jax import lax
from jax.experimental import pallas as pl
from jax.experimental.pallas import tpu as pltpu
from jax.sharding import PartitionSpec as P

MESH = pl.DeviceIdType.MESH
F32 = jnp.float32
BF16 = jnp.bfloat16

NX = 4
NZ = 8
NBAND = 8
PROJ = 512
ATOMS = 64
NSPEC = 4
KMAX = 18
GL = 1024
BL = 256
CH = 128
NCH = BL // CH
QR = PROJ // NX
SR = QR // NZ

FAR_FIRST = (4, 3, 5, 2, 6, 1, 7)
NEAR_FIRST = (1, 7, 2, 6, 3, 5, 4)

KINETIC_SCALE = 0.005
EPSILON = 1e-6

SIN_C = (3.141592653589793, -5.16771278004997, 2.550164039877345, -0.5992645293207921, 0.08214588661112823, -0.00737043094571435, 0.00046630280576761255)
COS_C = (1.0, -4.934802200544679, 4.058712126416768, -1.3352627688545893, 0.2353306303588935, -0.02580689139001406, 0.0019295743094039231)


def split(x):
    hi = x.astype(BF16)
    return hi, (x - hi.astype(F32)).astype(BF16)


def dot(a, b):
    return jnp.dot(a, b, preferred_element_type=F32)


def dot3(ah, al, bh, bl):
    return dot(ah, bh) + dot(al, bh) + dot(ah, bl)


def horner(coeffs, x):
    acc = jnp.full_like(x, coeffs[-1])
    for c in coeffs[-2::-1]:
        acc = acc * x + c
    return acc


def iota(shape, dim):
    return lax.broadcasted_iota(jnp.int32, shape, dim)


def kernel(waves, miller_in, pos_in, ff_in, coup_in, spec_in, size_in, occ_in,
           res, est_to, en_out,
           psi, bh, bl, th, tl, vh, vl, dh, dl, mh, ml,
           ffs, ffk, ctk, stk, cks, ckk, kcol, pbuf, xr, q, zr, full, rbuf,
           knx, knz, kna, ebuf, miller, pos, ff, coup, spec, size, occ, est_out,
           in_sem, est_sem, out_sem, sent, xr_sem, zr_sem, za_sem, xa_sem, kn_sem):
    gi = lax.axis_index("ga")
    band = lax.axis_index("band")
    z = lax.div(gi, NX)
    x = lax.rem(gi, NX)
    r, o, l = (lax.rem(x + k, NX) for k in (1, 2, 3))

    def at_x(xx):
        return {"ga": z * NX + xx}

    def at_z(k):
        return {"ga": lax.rem(z + k, NZ) * NX + x}

    def at_band(k):
        return {"band": lax.rem(band + k, NBAND)}

    smalls = [
        pltpu.make_async_copy(a, b, in_sem.at[2 + i])
        for i, (a, b) in enumerate((
            (size_in, size), (spec_in, spec), (pos_in, pos), (miller_in, miller),
            (ff_in, ff), (coup_in, coup), (occ_in, occ),
        ))
    ]
    loads = [pltpu.make_async_copy(waves.at[i], psi.at[i], in_sem.at[i]) for i in range(2)]
    for c in smalls + loads:
        c.start()

    barrier = pltpu.get_barrier_semaphore()
    peers = [at_x(r), at_x(l), at_x(o)] + [at_z(k) for k in range(1, NZ)] + [at_band(k) for k in range(1, NBAND)]
    for p in peers:
        pl.semaphore_signal(barrier, inc=1, device_id=p, device_id_type=MESH)

    def remote(src, dst, where, recv_sem, send_sem=None):
        copy = pltpu.make_async_remote_copy(
            src_ref=src, dst_ref=dst, send_sem=sent.at[0] if send_sem is None else send_sem,
            recv_sem=recv_sem, device_id=where, device_id_type=MESH,
        )
        copy.start()
        return copy

    def arrived(ref, sem):
        pltpu.make_async_copy(ref, ref, sem).wait()

    for c in smalls:
        c.wait()
    size_row = size[...].astype(F32)
    spec_row = spec[...].astype(F32)
    i0, i1 = iota((ATOMS, ATOMS), 0), iota((ATOMS, ATOMS), 1)
    size_col = jnp.sum(jnp.where(i0 == i1, size_row, 0.0), axis=1, keepdims=True)
    end_row = jnp.sum(jnp.where(i0 <= i1, size_col, 0.0), axis=0, keepdims=True)
    end_col = jnp.sum(jnp.where(i1 <= i0, size_row, 0.0), axis=1, keepdims=True)
    start_row = end_row - size_row
    start_col = end_col - size_col
    p_col = iota((PROJ, ATOMS), 0).astype(F32)
    own = (p_col >= start_row) & (p_col < end_row)
    atom_row = iota((1, ATOMS), 1).astype(F32)
    owner_col = jnp.sum(jnp.where(own, atom_row, 0.0), axis=1, keepdims=True)
    row_col = jnp.sum(jnp.where(own, spec_row + NSPEC * (p_col - start_row), 0.0), axis=1, keepdims=True)
    lane = iota((PROJ, 256), 1)
    row_hot = jnp.where((lane & 127).astype(F32) == row_col, 1.0, 0.0).astype(BF16)
    own_hot = jnp.where((lane[:, :128] & 63).astype(F32) == owner_col, 1.0, 0.0).astype(BF16)

    ffs[72:80, :] = jnp.zeros((8, GL), F32)
    for k in range(KMAX):
        ffs[k * NSPEC:(k + 1) * NSPEC, :] = ff[k]
    for g in range(0, 256, 128):
        ffk[g + 80:g + 128, :] = jnp.zeros((48, GL), BF16)
    ffk[0:80, :], ffk[128:208, :] = split(ffs[...])
    pos_col = [
        jnp.sum(jnp.where(i0 == i1, pos[i:i + 1, :], 0.0), axis=1, keepdims=True) for i in range(3)
    ]
    m = miller[...].astype(F32)
    for g in range(0, GL, 256):
        mg = m[:, g:g + 256]
        turns = pos_col[0] * mg[0:1] + pos_col[1] * mg[1:2] + pos_col[2] * mg[2:3]
        turns = turns - jnp.round(turns)
        t2 = turns * turns
        sh = horner(SIN_C, t2) * turns
        ch = horner(COS_C, t2)
        for dst, val in ((ctk, 1.0 - 2.0 * (sh * sh)), (stk, 2.0 * (sh * ch))):
            a, b = split(val)
            dst[0:64, g:g + 256] = a
            dst[64:128, g:g + 256] = b
        radial = dot(row_hot, ffk[:, g:g + 256])
        for base, tab, sign in ((0, ctk, 1.0), (GL, stk, -1.0)):
            b = radial * dot(own_hot, tab[:, g:g + 256])
            b = b if sign > 0 else -b
            a, b = split(b)
            bh[:, base + g:base + g + 256] = a
            bl[:, base + g:base + g + 256] = b
    ksum = m[0:1] * m[0:1] + m[1:2] * m[1:2] + m[2:3] * m[2:3]
    krow = jnp.broadcast_to(0.5 * KINETIC_SCALE * ksum, (128, GL))
    for g in range(0, GL, 128):
        kcol[g:g + 128, :] = jnp.transpose(krow[:, g:g + 128])

    for c in loads:
        c.wait()

    def project(c):
        cols = slice(c * CH, (c + 1) * CH)
        rows = 256
        kin = jnp.zeros((1, CH), F32)
        nrm = jnp.zeros((1, CH), F32)
        for g in range(0, GL, rows):
            pr = psi[0, g:g + rows, cols]
            pi = psi[1, g:g + rows, cols]
            den = pr * pr + pi * pi
            nrm = nrm + jnp.sum(den, axis=0, keepdims=True)
            kin = kin + jnp.sum(kcol[g:g + rows, :] * den, axis=0, keepdims=True)
            for buf, (a, b) in zip((vh, vl), zip(split(pr), split(pi))):
                buf[g:g + rows, 0:CH] = a
                buf[g:g + rows, CH:2 * CH] = b
                buf[GL + g:GL + g + rows, 0:CH] = b
                buf[GL + g:GL + g + rows, CH:2 * CH] = -a
        return kin, nrm

    def projected(c, rows):
        p = dot3(bh[rows, :], bl[rows, :], vh[...], vl[...])
        pbuf[c, 0, rows, :] = p[:, :CH]
        pbuf[c, 1, rows, :] = p[:, CH:]

    def rows_of(xx, zz):
        return pl.ds(pl.multiple_of(xx * QR + zz * SR, SR), SR)

    def z_at(k):
        return lax.rem(z + k, NZ)

    def x_at(k):
        return lax.rem(x + k, NX)

    def x_first(c, to=(2, 1, 3)):
        for k in FAR_FIRST + (0,):
            for d in to:
                part = pbuf.at[c, :, rows_of(x_at(d), z_at(k)), :]
                remote(part, xr.at[c, k, d - 1], at_x(x_at(d)), xr_sem.at[c, k])

    def z_first(c):
        for k in FAR_FIRST + (0,):
            arrived(xr.at[c, k], xr_sem.at[c, k])
            q[c, k] = pbuf[c, :, rows_of(x, z_at(k)), :] + xr[c, k, 0] + xr[c, k, 1] + xr[c, k, 2]
            if k:
                remote(q.at[c, k], zr.at[c, k - 1], at_z(k), zr_sem.at[c])

    mine = rows_of(x, z)

    def spread(c, zz):
        part = full.at[c, :, rows_of(x, zz), :]
        for d in (2, 1, 3):
            remote(part, part, at_x(x_at(d)), xa_sem.at[c])

    def z_back(c):
        arrived(zr.at[c], zr_sem.at[c])
        share = q[c, 0]
        for k in range(NZ - 1):
            share = share + zr[c, k]
        full[c, :, mine, :] = share
        part = full.at[c, :, mine, :]
        spread(c, z)
        return {k: remote(part, part, at_z(k), za_sem.at[c, k - 1]) for k in NEAR_FIRST}

    def x_back(c, back):
        for k in NEAR_FIRST:
            back[k].wait_recv()
            spread(c, z_at(NZ - k))

    kn0 = project(0)
    for i, d in enumerate((2, 1, 3, 0)):
        projected(0, pl.ds(pl.multiple_of(x_at(d) * QR, QR), QR))
        if i == 0:
            pl.semaphore_wait(barrier, len(peers))
        if d:
            x_first(0, (d,))
    kn1 = project(1)
    projected(1, slice(0, PROJ))
    x_first(1)

    tile_row = iota((8, CH), 0)
    kn = jnp.zeros((8, CH), F32)
    for i, v in enumerate((kn0[0], kn0[1], kn1[0], kn1[1])):
        kn = jnp.where(tile_row == i, v, kn)
    knx[x] = kn
    for k in (r, l, o):
        remote(knx.at[x], knx.at[x], at_x(k), kn_sem.at[0], sent.at[1])

    z_first(0)
    cks[...] = jnp.zeros_like(cks)
    for k in range(KMAX):
        cks[k * NSPEC:(k + 1) * NSPEC, 0:KMAX] = coup[k]
    ckk[0:128, :], ckk[128:256, :] = split(cks[...])
    q_row = iota((ATOMS, PROJ), 1).astype(F32)
    own_t = (q_row >= start_col) & (q_row < end_col)
    atom_col = iota((ATOMS, 1), 0).astype(F32)
    owner_row = jnp.sum(jnp.where(own_t, atom_col, 0.0), axis=0, keepdims=True)
    chan_row = jnp.sum(jnp.where(own_t, q_row - start_col, 0.0), axis=0, keepdims=True)
    chan_hot = jnp.where(iota((128, PROJ), 0).astype(F32) == chan_row, 1.0, 0.0).astype(BF16)
    same = owner_col == owner_row
    for dst, part in ((dh, row_hot[:, :128]), (dl, row_hot[:, 128:])):
        base = 0 if dst is dh else 128
        table = dot(part, ckk[base:base + 128, :]).astype(BF16)
        dst[...] = jnp.where(same, dot(table, chan_hot), 0.0).astype(BF16)

    def turned(g):
        for src, dst in ((bh, th), (bl, tl)):
            for half in range(2):
                dst[g:g + 256, half * PROJ:(half + 1) * PROJ] = jnp.transpose(
                    src[:, half * GL + g:half * GL + g + 256]
                )

    for g in range(0, GL, 256):
        turned(g)


    z_first(1)
    arrived(knx.at[0:NX - 1], kn_sem.at[0])
    knz[z] = knx[0] + knx[1] + knx[2] + knx[3]
    for k in range(1, NZ):
        remote(knz.at[z], knz.at[z], at_z(k), kn_sem.at[1], sent.at[1])


    back0 = z_back(0)
    x_back(0, back0)
    back1 = z_back(1)
    x_back(1, back1)
    arrived(knz.at[0:NZ - 1], kn_sem.at[1])
    tot = knz[0]
    for k in range(1, NZ):
        tot = tot + knz[k]
    kna[...] = tot

    def finish(c):
        arrived(full.at[c, :, 0:PROJ - QR, :], xa_sem.at[c])
        cols = slice(c * CH, (c + 1) * CH)
        for i in range(2):
            a, b = split(full[c, i])
            mh[c, 0:PROJ, i * CH:(i + 1) * CH] = a
            ml[c, 0:PROJ, i * CH:(i + 1) * CH] = b
        mix = dot3(dh[...], dl[...], mh[c, 0:PROJ, :], ml[c, 0:PROJ, :])
        mr, mi = mix[:, :CH], mix[:, CH:]
        nonlocal_ = jnp.sum(full[c, 0] * mr + full[c, 1] * mi, axis=0, keepdims=True)
        for buf, (a, b) in zip((mh, ml), zip(split(mr), split(mi))):
            buf[c, 0:PROJ, 0:CH] = a
            buf[c, 0:PROJ, CH:2 * CH] = b
            buf[c, PROJ:2 * PROJ, 0:CH] = -b
            buf[c, PROJ:2 * PROJ, CH:2 * CH] = a
        kin, nrm = kna[2 * c:2 * c + 1, :], kna[2 * c + 1:2 * c + 2, :]
        est = (kin + nonlocal_) / (nrm + EPSILON)
        est_out[:, cols] = est
        energy = occ[:, cols] * nonlocal_ / (nrm + EPSILON)
        return est, energy

    def residual(c, est):
        cols = slice(c * CH, (c + 1) * CH)
        out = []
        acc = dot3(th[...], tl[...], mh[c], ml[c])
        for i in range(2):
            rbuf[i, :, cols] = (kcol[...] - est) * psi[i, :, cols] + acc[:, i * CH:(i + 1) * CH]
            copy = pltpu.make_async_copy(rbuf.at[i, :, cols], res.at[i, :, cols], out_sem.at[c, i])
            copy.start()
            out.append(copy)
        return out

    est0, en0 = finish(0)
    est1, en1 = finish(1)
    ebuf[band] = jnp.broadcast_to(en0 + en1, (8, CH))
    for k in range(1, NBAND):
        remote(ebuf.at[band], ebuf.at[band], at_band(k), kn_sem.at[2], sent.at[1])
    est_copy = pltpu.make_async_copy(est_out, est_to, est_sem)
    est_copy.start()
    outs = residual(0, est0) + residual(1, est1) + [est_copy]
    arrived(ebuf.at[0:NBAND - 1], kn_sem.at[2])
    total = ebuf[0]
    for k in range(1, NBAND):
        total = total + ebuf[k]
    en_out[0, 0] = jnp.sum(total[0:1, :])
    arrived(rbuf.at[:, 0:NPIECE * 8, :], sent.at[0])
    arrived(pbuf.at[0, 0, 0:NTILE * 8, :], sent.at[1])
    for w in outs:
        w.wait()


NPIECE = NCH * (24 + 7 + 7 + 24)
NTILE = 3 + 7 + 7


def on_device(waves, miller, positions, form_factors, coupling, species, block_sizes, occupation):
    anywhere = pl.BlockSpec(memory_space=pl.ANY)
    res, est, en = pl.pallas_call(
        kernel,
        out_shape=(
            jax.ShapeDtypeStruct((2, GL, BL), F32),
            jax.ShapeDtypeStruct((1, BL), F32),
            jax.ShapeDtypeStruct((1, 1), F32),
        ),
        in_specs=[anywhere] * 8,
        out_specs=(
            anywhere,
            anywhere,
            pl.BlockSpec(memory_space=pltpu.SMEM),
        ),
        scratch_shapes=[
            pltpu.VMEM((2, GL, BL), F32),
            pltpu.VMEM((PROJ, 2 * GL), BF16),
            pltpu.VMEM((PROJ, 2 * GL), BF16),
            pltpu.VMEM((GL, 2 * PROJ), BF16),
            pltpu.VMEM((GL, 2 * PROJ), BF16),
            pltpu.VMEM((2 * GL, 2 * CH), BF16),
            pltpu.VMEM((2 * GL, 2 * CH), BF16),
            pltpu.VMEM((PROJ, PROJ), BF16),
            pltpu.VMEM((PROJ, PROJ), BF16),
            pltpu.VMEM((NCH, 2 * PROJ, 2 * CH), BF16),
            pltpu.VMEM((NCH, 2 * PROJ, 2 * CH), BF16),
            pltpu.VMEM((80, GL), F32),
            pltpu.VMEM((256, GL), BF16),
            pltpu.VMEM((128, GL), BF16),
            pltpu.VMEM((128, GL), BF16),
            pltpu.VMEM((128, 128), F32),
            pltpu.VMEM((256, 128), BF16),
            pltpu.VMEM((GL, CH), F32),
            pltpu.VMEM((NCH, 2, PROJ, CH), F32),
            pltpu.VMEM((NCH, NZ, NX - 1, 2, SR, CH), F32),
            pltpu.VMEM((NCH, NZ, 2, SR, CH), F32),
            pltpu.VMEM((NCH, NZ - 1, 2, SR, CH), F32),
            pltpu.VMEM((NCH, 2, PROJ, CH), F32),
            pltpu.VMEM((2, GL, BL), F32),
            pltpu.VMEM((NX, 8, CH), F32),
            pltpu.VMEM((NZ, 8, CH), F32),
            pltpu.VMEM((8, CH), F32),
            pltpu.VMEM((NBAND, 8, CH), F32),
            pltpu.VMEM((3, GL), jnp.int32),
            pltpu.VMEM((3, ATOMS), F32),
            pltpu.VMEM((KMAX, NSPEC, GL), F32),
            pltpu.VMEM((KMAX, NSPEC, KMAX), F32),
            pltpu.VMEM((1, ATOMS), jnp.int32),
            pltpu.VMEM((1, ATOMS), jnp.int32),
            pltpu.VMEM((1, BL), F32),
            pltpu.VMEM((1, BL), F32),
            pltpu.SemaphoreType.DMA((9,)),
            pltpu.SemaphoreType.DMA,
            pltpu.SemaphoreType.DMA((NCH, 2)),
            pltpu.SemaphoreType.DMA((2,)),
            pltpu.SemaphoreType.DMA((NCH, NZ)),
            pltpu.SemaphoreType.DMA((NCH,)),
            pltpu.SemaphoreType.DMA((NCH, NZ - 1)),
            pltpu.SemaphoreType.DMA((NCH,)),
            pltpu.SemaphoreType.DMA((3,)),
        ],
        compiler_params=pltpu.CompilerParams(
            collective_id=0, has_side_effects=True, vmem_limit_bytes=60000 * 1024
        ),
    )(
        waves, miller, positions.T, form_factors.transpose(1, 0, 2), coupling.transpose(1, 0, 2),
        species.reshape(1, -1), block_sizes.reshape(1, -1), occupation.reshape(1, -1),
    )
    return res, est.reshape(BL), en.reshape(())


def solution(mesh):
    in_specs = (
        P(None, "ga", "band"),
        P(None, "ga"),
        P(),
        P(None, None, "ga"),
        P(),
        P(),
        P(),
        P("band"),
    )
    out_specs = (P(None, "ga", "band"), P("band"), P())
    return jax.shard_map(
        on_device, mesh=mesh, in_specs=in_specs, out_specs=out_specs, check_vma=False
    )
```

```python
import jax
import jax.numpy as jnp
from jax import lax
from jax.experimental import pallas as pl
from jax.experimental.pallas import tpu as pltpu
from jax.sharding import PartitionSpec as P

MESH = pl.DeviceIdType.MESH
F32 = jnp.float32
BF16 = jnp.bfloat16

NX = 4
NZ = 8
NBAND = 8
PROJ = 512
ATOMS = 64
NSPEC = 4
KMAX = 18
GL = 1024
BL = 256
CH = 128
NCH = BL // CH
QR = PROJ // NX
SR = QR // NZ

FAR_FIRST = (4, 3, 5, 2, 6, 1, 7)
NEAR_FIRST = (1, 7, 2, 6, 3, 5, 4)

KINETIC_SCALE = 0.005
EPSILON = 1e-6

SIN_C = (3.141592653589793, -5.16771278004997, 2.550164039877345, -0.5992645293207921, 0.08214588661112823, -0.00737043094571435, 0.00046630280576761255)
COS_C = (1.0, -4.934802200544679, 4.058712126416768, -1.3352627688545893, 0.2353306303588935, -0.02580689139001406, 0.0019295743094039231)


def split(x):
    hi = x.astype(BF16)
    return hi, (x - hi.astype(F32)).astype(BF16)


def dot(a, b):
    return jnp.dot(a, b, preferred_element_type=F32)


def dot3(ah, al, bh, bl):
    return dot(ah, bh) + dot(al, bh) + dot(ah, bl)


def horner(coeffs, x):
    acc = jnp.full_like(x, coeffs[-1])
    for c in coeffs[-2::-1]:
        acc = acc * x + c
    return acc


def iota(shape, dim):
    return lax.broadcasted_iota(jnp.int32, shape, dim)


def kernel(waves, miller_in, pos_in, ff_in, coup_in, spec_in, size_in, occ_in,
           res, est_to, en_out,
           psi, bh, bl, th, tl, vh, vl, dhl, mh, ml,
           ffs, ffk, ctk, stk, cks, ckk, kcol, pbuf, xr, q, zr, full, rbuf,
           knx, knz, kna, ebuf, miller, pos, ff, coup, spec, size, occ, est_out,
           in_sem, est_sem, out_sem, sent, xr_sem, zr_sem, za_sem, xa_sem, kn_sem):
    gi = lax.axis_index("ga")
    band = lax.axis_index("band")
    z = lax.div(gi, NX)
    x = lax.rem(gi, NX)
    r, o, l = (lax.rem(x + k, NX) for k in (1, 2, 3))

    def at_x(xx):
        return {"ga": z * NX + xx}

    def at_z(k):
        return {"ga": lax.rem(z + k, NZ) * NX + x}

    def at_band(k):
        return {"band": lax.rem(band + k, NBAND)}

    smalls = [
        pltpu.make_async_copy(a, b, in_sem.at[2 + i])
        for i, (a, b) in enumerate((
            (size_in, size), (spec_in, spec), (pos_in, pos), (miller_in, miller),
            (ff_in, ff), (coup_in, coup), (occ_in, occ),
        ))
    ]
    loads = [pltpu.make_async_copy(waves.at[i], psi.at[i], in_sem.at[i]) for i in range(2)]
    for c in smalls + loads:
        c.start()

    barrier = pltpu.get_barrier_semaphore()
    peers = [at_x(r), at_x(l), at_x(o)] + [at_z(k) for k in range(1, NZ)] + [at_band(k) for k in range(1, NBAND)]
    for p in peers:
        pl.semaphore_signal(barrier, inc=1, device_id=p, device_id_type=MESH)

    def remote(src, dst, where, recv_sem, send_sem=None):
        copy = pltpu.make_async_remote_copy(
            src_ref=src, dst_ref=dst, send_sem=sent.at[0] if send_sem is None else send_sem,
            recv_sem=recv_sem, device_id=where, device_id_type=MESH,
        )
        copy.start()
        return copy

    def arrived(ref, sem):
        pltpu.make_async_copy(ref, ref, sem).wait()

    for c in smalls:
        c.wait()
    size_row = size[...].astype(F32)
    spec_row = spec[...].astype(F32)
    i0, i1 = iota((ATOMS, ATOMS), 0), iota((ATOMS, ATOMS), 1)
    size_col = jnp.sum(jnp.where(i0 == i1, size_row, 0.0), axis=1, keepdims=True)
    end_row = jnp.sum(jnp.where(i0 <= i1, size_col, 0.0), axis=0, keepdims=True)
    end_col = jnp.sum(jnp.where(i1 <= i0, size_row, 0.0), axis=1, keepdims=True)
    start_row = end_row - size_row
    start_col = end_col - size_col
    p_col = iota((PROJ, ATOMS), 0).astype(F32)
    own = (p_col >= start_row) & (p_col < end_row)
    atom_row = iota((1, ATOMS), 1).astype(F32)
    owner_col = jnp.sum(jnp.where(own, atom_row, 0.0), axis=1, keepdims=True)
    row_col = jnp.sum(jnp.where(own, spec_row + NSPEC * (p_col - start_row), 0.0), axis=1, keepdims=True)
    lane = iota((PROJ, 256), 1)
    row_hot = jnp.where((lane & 127).astype(F32) == row_col, 1.0, 0.0).astype(BF16)
    own_hot = jnp.where((lane[:, :128] & 63).astype(F32) == owner_col, 1.0, 0.0).astype(BF16)

    ffs[72:80, :] = jnp.zeros((8, GL), F32)
    for k in range(KMAX):
        ffs[k * NSPEC:(k + 1) * NSPEC, :] = ff[k]
    for g in range(0, 256, 128):
        ffk[g + 80:g + 128, :] = jnp.zeros((48, GL), BF16)
    ffk[0:80, :], ffk[128:208, :] = split(ffs[...])
    pos_col = [
        jnp.sum(jnp.where(i0 == i1, pos[i:i + 1, :], 0.0), axis=1, keepdims=True) for i in range(3)
    ]
    m = miller[...].astype(F32)
    for g in range(0, GL, 256):
        mg = m[:, g:g + 256]
        turns = pos_col[0] * mg[0:1] + pos_col[1] * mg[1:2] + pos_col[2] * mg[2:3]
        turns = turns - jnp.round(turns)
        t2 = turns * turns
        sh = horner(SIN_C, t2) * turns
        ch = horner(COS_C, t2)
        for dst, val in ((ctk, 1.0 - 2.0 * (sh * sh)), (stk, 2.0 * (sh * ch))):
            a, b = split(val)
            dst[0:64, g:g + 256] = a
            dst[64:128, g:g + 256] = b
        radial = dot(row_hot, ffk[:, g:g + 256])
        for base, tab, sign in ((0, ctk, 1.0), (GL, stk, -1.0)):
            b = radial * dot(own_hot, tab[:, g:g + 256])
            b = b if sign > 0 else -b
            a, b = split(b)
            bh[:, base + g:base + g + 256] = a
            bl[:, base + g:base + g + 256] = b
    ksum = m[0:1] * m[0:1] + m[1:2] * m[1:2] + m[2:3] * m[2:3]
    krow = jnp.broadcast_to(0.5 * KINETIC_SCALE * ksum, (128, GL))
    for g in range(0, GL, 128):
        kcol[g:g + 128, :] = jnp.transpose(krow[:, g:g + 128])

    for c in loads:
        c.wait()

    def project(c):
        cols = slice(c * CH, (c + 1) * CH)
        rows = 256
        kin = jnp.zeros((1, CH), F32)
        nrm = jnp.zeros((1, CH), F32)
        for g in range(0, GL, rows):
            pr = psi[0, g:g + rows, cols]
            pi = psi[1, g:g + rows, cols]
            den = pr * pr + pi * pi
            nrm = nrm + jnp.sum(den, axis=0, keepdims=True)
            kin = kin + jnp.sum(kcol[g:g + rows, :] * den, axis=0, keepdims=True)
            for buf, (a, b) in zip((vh, vl), zip(split(pr), split(pi))):
                buf[g:g + rows, 0:CH] = a
                buf[g:g + rows, CH:2 * CH] = b
                buf[GL + g:GL + g + rows, 0:CH] = b
                buf[GL + g:GL + g + rows, CH:2 * CH] = -a
        return kin, nrm

    def projected(c, rows):
        p = dot3(bh[rows, :], bl[rows, :], vh[...], vl[...])
        pbuf[c, 0, rows, :] = p[:, :CH]
        pbuf[c, 1, rows, :] = p[:, CH:]

    def rows_of(xx, zz):
        return pl.ds(pl.multiple_of(xx * QR + zz * SR, SR), SR)

    def z_at(k):
        return lax.rem(z + k, NZ)

    def x_at(k):
        return lax.rem(x + k, NX)

    def x_first(c, to=(2, 1, 3)):
        for k in FAR_FIRST + (0,):
            for d in to:
                part = pbuf.at[c, :, rows_of(x_at(d), z_at(k)), :]
                remote(part, xr.at[c, k, d - 1], at_x(x_at(d)), xr_sem.at[c, k])

    def z_first(c):
        for k in FAR_FIRST + (0,):
            arrived(xr.at[c, k], xr_sem.at[c, k])
            q[c, k] = pbuf[c, :, rows_of(x, z_at(k)), :] + xr[c, k, 0] + xr[c, k, 1] + xr[c, k, 2]
            if k:
                remote(q.at[c, k], zr.at[c, k - 1], at_z(k), zr_sem.at[c])

    mine = rows_of(x, z)

    def spread(c, zz):
        part = full.at[c, :, rows_of(x, zz), :]
        for d in (2, 1, 3):
            remote(part, part, at_x(x_at(d)), xa_sem.at[c])

    def z_back(c):
        arrived(zr.at[c], zr_sem.at[c])
        share = q[c, 0]
        for k in range(NZ - 1):
            share = share + zr[c, k]
        full[c, :, mine, :] = share
        part = full.at[c, :, mine, :]
        spread(c, z)
        return {k: remote(part, part, at_z(k), za_sem.at[c, k - 1]) for k in NEAR_FIRST}

    def x_back(c, back):
        for k in NEAR_FIRST:
            back[k].wait_recv()
            spread(c, z_at(NZ - k))

    kn0 = project(0)
    for i, d in enumerate((2, 1, 3, 0)):
        projected(0, pl.ds(pl.multiple_of(x_at(d) * QR, QR), QR))
        if i == 0:
            pl.semaphore_wait(barrier, len(peers))
        if d:
            x_first(0, (d,))
    kn1 = project(1)
    projected(1, slice(0, PROJ))
    x_first(1)

    tile_row = iota((8, CH), 0)
    kn = jnp.zeros((8, CH), F32)
    for i, v in enumerate((kn0[0], kn0[1], kn1[0], kn1[1])):
        kn = jnp.where(tile_row == i, v, kn)
    knx[x] = kn
    for k in (r, l, o):
        remote(knx.at[x], knx.at[x], at_x(k), kn_sem.at[0], sent.at[1])

    z_first(0)
    cks[...] = jnp.zeros_like(cks)
    for k in range(KMAX):
        cks[k * NSPEC:(k + 1) * NSPEC, 0:KMAX] = coup[k]
    ckk[0:128, :], ckk[128:256, :] = split(cks[...])
    q_row = iota((ATOMS, PROJ), 1).astype(F32)
    own_t = (q_row >= start_col) & (q_row < end_col)
    atom_col = iota((ATOMS, 1), 0).astype(F32)
    owner_row = jnp.sum(jnp.where(own_t, atom_col, 0.0), axis=0, keepdims=True)
    chan_row = jnp.sum(jnp.where(own_t, q_row - start_col, 0.0), axis=0, keepdims=True)
    chan_hot = jnp.where(iota((128, PROJ), 0).astype(F32) == chan_row, 1.0, 0.0).astype(BF16)
    same = owner_col == owner_row
    for at, part in ((0, row_hot[:, :128]), (PROJ, row_hot[:, 128:])):
        base = 128 if at else 0
        table = dot(part, ckk[base:base + 128, :]).astype(BF16)
        dhl[at:at + PROJ, :] = jnp.where(same, dot(table, chan_hot), 0.0).astype(BF16)

    def turned(g):
        for src, dst in ((bh, th), (bl, tl)):
            for half in range(2):
                dst[g:g + 256, half * PROJ:(half + 1) * PROJ] = jnp.transpose(
                    src[:, half * GL + g:half * GL + g + 256]
                )

    for g in range(0, GL, 256):
        turned(g)


    z_first(1)
    arrived(knx.at[0:NX - 1], kn_sem.at[0])
    knz[z] = knx[0] + knx[1] + knx[2] + knx[3]
    for k in range(1, NZ):
        remote(knz.at[z], knz.at[z], at_z(k), kn_sem.at[1], sent.at[1])


    back0 = z_back(0)
    x_back(0, back0)
    back1 = z_back(1)
    x_back(1, back1)
    arrived(knz.at[0:NZ - 1], kn_sem.at[1])
    tot = knz[0]
    for k in range(1, NZ):
        tot = tot + knz[k]
    kna[...] = tot

    def finish(c):
        arrived(full.at[c, :, 0:PROJ - QR, :], xa_sem.at[c])
        cols = slice(c * CH, (c + 1) * CH)
        for i in range(2):
            a, b = split(full[c, i])
            mh[c, 0:PROJ, i * CH:(i + 1) * CH] = a
            ml[c, 0:PROJ, i * CH:(i + 1) * CH] = b
        both = dot(dhl[...], mh[c, 0:PROJ, :])
        mix = both[:PROJ] + both[PROJ:] + dot(dhl[0:PROJ, :], ml[c, 0:PROJ, :])
        mr, mi = mix[:, :CH], mix[:, CH:]
        nonlocal_ = jnp.sum(full[c, 0] * mr + full[c, 1] * mi, axis=0, keepdims=True)
        for buf, (a, b) in zip((mh, ml), zip(split(mr), split(mi))):
            buf[c, 0:PROJ, 0:CH] = a
            buf[c, 0:PROJ, CH:2 * CH] = b
            buf[c, PROJ:2 * PROJ, 0:CH] = -b
            buf[c, PROJ:2 * PROJ, CH:2 * CH] = a
        kin, nrm = kna[2 * c:2 * c + 1, :], kna[2 * c + 1:2 * c + 2, :]
        est = (kin + nonlocal_) / (nrm + EPSILON)
        est_out[:, cols] = est
        energy = occ[:, cols] * nonlocal_ / (nrm + EPSILON)
        return est, energy

    def residual(c, est):
        cols = slice(c * CH, (c + 1) * CH)
        out = []
        acc = dot3(th[...], tl[...], mh[c], ml[c])
        for i in range(2):
            rbuf[i, :, cols] = (kcol[...] - est) * psi[i, :, cols] + acc[:, i * CH:(i + 1) * CH]
            copy = pltpu.make_async_copy(rbuf.at[i, :, cols], res.at[i, :, cols], out_sem.at[c, i])
            copy.start()
            out.append(copy)
        return out

    est0, en0 = finish(0)
    est1, en1 = finish(1)
    ebuf[band] = jnp.broadcast_to(en0 + en1, (8, CH))
    for k in range(1, NBAND):
        remote(ebuf.at[band], ebuf.at[band], at_band(k), kn_sem.at[2], sent.at[1])
    est_copy = pltpu.make_async_copy(est_out, est_to, est_sem)
    est_copy.start()
    outs = residual(0, est0) + residual(1, est1) + [est_copy]
    arrived(ebuf.at[0:NBAND - 1], kn_sem.at[2])
    total = ebuf[0]
    for k in range(1, NBAND):
        total = total + ebuf[k]
    en_out[0, 0] = jnp.sum(total[0:1, :])
    arrived(rbuf.at[:, 0:NPIECE * 8, :], sent.at[0])
    arrived(pbuf.at[0, 0, 0:NTILE * 8, :], sent.at[1])
    for w in outs:
        w.wait()


NPIECE = NCH * (24 + 7 + 7 + 24)
NTILE = 3 + 7 + 7


def on_device(waves, miller, positions, form_factors, coupling, species, block_sizes, occupation):
    anywhere = pl.BlockSpec(memory_space=pl.ANY)
    res, est, en = pl.pallas_call(
        kernel,
        out_shape=(
            jax.ShapeDtypeStruct((2, GL, BL), F32),
            jax.ShapeDtypeStruct((1, BL), F32),
            jax.ShapeDtypeStruct((1, 1), F32),
        ),
        in_specs=[anywhere] * 8,
        out_specs=(
            anywhere,
            anywhere,
            pl.BlockSpec(memory_space=pltpu.SMEM),
        ),
        scratch_shapes=[
            pltpu.VMEM((2, GL, BL), F32),
            pltpu.VMEM((PROJ, 2 * GL), BF16),
            pltpu.VMEM((PROJ, 2 * GL), BF16),
            pltpu.VMEM((GL, 2 * PROJ), BF16),
            pltpu.VMEM((GL, 2 * PROJ), BF16),
            pltpu.VMEM((2 * GL, 2 * CH), BF16),
            pltpu.VMEM((2 * GL, 2 * CH), BF16),
            pltpu.VMEM((2 * PROJ, PROJ), BF16),
            pltpu.VMEM((NCH, 2 * PROJ, 2 * CH), BF16),
            pltpu.VMEM((NCH, 2 * PROJ, 2 * CH), BF16),
            pltpu.VMEM((80, GL), F32),
            pltpu.VMEM((256, GL), BF16),
            pltpu.VMEM((128, GL), BF16),
            pltpu.VMEM((128, GL), BF16),
            pltpu.VMEM((128, 128), F32),
            pltpu.VMEM((256, 128), BF16),
            pltpu.VMEM((GL, CH), F32),
            pltpu.VMEM((NCH, 2, PROJ, CH), F32),
            pltpu.VMEM((NCH, NZ, NX - 1, 2, SR, CH), F32),
            pltpu.VMEM((NCH, NZ, 2, SR, CH), F32),
            pltpu.VMEM((NCH, NZ - 1, 2, SR, CH), F32),
            pltpu.VMEM((NCH, 2, PROJ, CH), F32),
            pltpu.VMEM((2, GL, BL), F32),
            pltpu.VMEM((NX, 8, CH), F32),
            pltpu.VMEM((NZ, 8, CH), F32),
            pltpu.VMEM((8, CH), F32),
            pltpu.VMEM((NBAND, 8, CH), F32),
            pltpu.VMEM((3, GL), jnp.int32),
            pltpu.VMEM((3, ATOMS), F32),
            pltpu.VMEM((KMAX, NSPEC, GL), F32),
            pltpu.VMEM((KMAX, NSPEC, KMAX), F32),
            pltpu.VMEM((1, ATOMS), jnp.int32),
            pltpu.VMEM((1, ATOMS), jnp.int32),
            pltpu.VMEM((1, BL), F32),
            pltpu.VMEM((1, BL), F32),
            pltpu.SemaphoreType.DMA((9,)),
            pltpu.SemaphoreType.DMA,
            pltpu.SemaphoreType.DMA((NCH, 2)),
            pltpu.SemaphoreType.DMA((2,)),
            pltpu.SemaphoreType.DMA((NCH, NZ)),
            pltpu.SemaphoreType.DMA((NCH,)),
            pltpu.SemaphoreType.DMA((NCH, NZ - 1)),
            pltpu.SemaphoreType.DMA((NCH,)),
            pltpu.SemaphoreType.DMA((3,)),
        ],
        compiler_params=pltpu.CompilerParams(
            collective_id=0, has_side_effects=True, vmem_limit_bytes=60000 * 1024
        ),
    )(
        waves, miller, positions.T, form_factors.transpose(1, 0, 2), coupling.transpose(1, 0, 2),
        species.reshape(1, -1), block_sizes.reshape(1, -1), occupation.reshape(1, -1),
    )
    return res, est.reshape(BL), en.reshape(())


def solution(mesh):
    in_specs = (
        P(None, "ga", "band"),
        P(None, "ga"),
        P(),
        P(None, None, "ga"),
        P(),
        P(),
        P(),
        P("band"),
    )
    out_specs = (P(None, "ga", "band"), P("band"), P())
    return jax.shard_map(
        on_device, mesh=mesh, in_specs=in_specs, out_specs=out_specs, check_vma=False
    )
```
